32 devices in a mesh: rep: 4 (over x, y), dp: 8 (over z, core).
Axes of the slice: x: 2, y: 2, z: 4, core: 2. Of those that a mesh axis runs over, the one named last changes fastest.
Arguments:
- g_w_gate: bfloat16 [32, 2, 1280, 4480], P(('rep', 'dp')), parts along dimension 0
- g_w_up: bfloat16 [32, 2, 1280, 4480], P(('rep', 'dp')), parts along dimension 0
- g_w_down: bfloat16 [32, 2, 4480, 1280], P(('rep', 'dp')), parts along dimension 0
- w_gate: bfloat16 [2, 1280, 4480], replicated
- w_up: bfloat16 [2, 1280, 4480], replicated
- w_down: bfloat16 [2, 4480, 1280], replicated
- m_w_gate: float32 [2, 1280, 4480], P(None, 'dp')
- m_w_up: float32 [2, 1280, 4480], P(None, 'dp')
- m_w_down: float32 [2, 4480, 1280], P(None, 'dp')
- v_w_gate: float32 [2, 1280, 4480], P(None, 'dp')
- v_w_up: float32 [2, 1280, 4480], P(None, 'dp')
- v_w_down: float32 [2, 4480, 1280], P(None, 'dp')
Outputs:
- output 1: bfloat16 [8, 1280, 4480], P('rep'), parts along dimension 0
- output 2: bfloat16 [8, 1280, 4480], P('rep'), parts along dimension 0
- output 3: bfloat16 [8, 4480, 1280], P('rep'), parts along dimension 0
- output 4: float32 [8, 1280, 4480], P('rep', 'dp'), parts along dimension 0
- output 5: float32 [8, 1280, 4480], P('rep', 'dp'), parts along dimension 0
- output 6: float32 [8, 4480, 1280], P('rep', 'dp'), parts along dimension 0
- output 7: float32 [8, 1280, 4480], P('rep', 'dp'), parts along dimension 0
- output 8: float32 [8, 1280, 4480], P('rep', 'dp'), parts along dimension 0
- output 9: float32 [8, 4480, 1280], P('rep', 'dp'), parts along dimension 0
There are 4 independent parts. The reference program is written for one: setup_inputs(seed, part) draws one part's arguments, and reference() takes and returns one part's arrays. A program takes and returns all parts, laid end to end along the dimension named above; an argument that names none is the same for every part.
All inputs are finite; a program needn't handle non-finite values.
Results may differ from the reference program's by a relative error of at most 0.022.
Values are sent between devices in bfloat16 or wider.
A program may use at most 2 GiB of HBM per device.

```python
import jax
import jax.numpy as jnp
from jax import lax

DEVICES = 8
D = 1280
FF = 4480
LAYERS = 2
NAMES = ("w_gate", "w_up", "w_down")
SHAPES = {"w_gate": (LAYERS, D, FF), "w_up": (LAYERS, D, FF), "w_down": (LAYERS, FF, D)}


def setup_inputs(seed: int = 0, part: int = 0) -> dict:
    kz, *keys = jax.random.split(jax.random.key(seed), 1 + 5 * len(NAMES))
    loud = 2.0 ** jax.random.uniform(kz, (), jnp.float32, -1.0, 1.0)
    drawn = {}
    for name, key, both in zip(NAMES, keys[:3], keys[3:6], strict=True):
        own = jax.random.normal(jax.random.fold_in(key, part), (DEVICES, *SHAPES[name]), jnp.float32)
        shared = jax.random.normal(jax.random.fold_in(both, part), SHAPES[name], jnp.float32)
        drawn["g_" + name] = (loud * (0.7 * shared / DEVICES + 0.7 * own * DEVICES**-0.5)).astype(jnp.bfloat16)
    for name, key in zip(NAMES, keys[6:9], strict=True):
        drawn[name] = (jax.random.normal(key, SHAPES[name], jnp.float32) * SHAPES[name][1] ** -0.5).astype(jnp.bfloat16)
    for name, key in zip(NAMES, keys[9:12], strict=True):
        drawn["m_" + name] = loud * 0.5 * jax.random.normal(key, SHAPES[name], jnp.float32)
    for name, key in zip(NAMES, keys[12:15], strict=True):
        drawn["v_" + name] = loud * loud * jax.random.uniform(key, SHAPES[name], jnp.float32, 0.5, 1.5)
    return drawn


def adamw(w, m, v, g):
    m = 0.9 * m + 0.1 * g
    v = 0.95 * v + 0.05 * g * g
    step = m * lax.rsqrt(v + 1e-8) + 0.1 * w
    return (w - 0.02 * step).astype(jnp.bfloat16), m, v


def reference(g_w_gate, g_w_up, g_w_down, w_gate, w_up, w_down, m_w_gate, m_w_up, m_w_down, v_w_gate, v_w_up, v_w_down):
    def total(terms):
        return lax.scan(lambda so_far, term: (so_far + term.astype(jnp.float32), None), jnp.zeros(terms.shape[1:], jnp.float32), terms)[0]

    gradients = [total(terms).astype(jnp.bfloat16).astype(jnp.float32) for terms in (g_w_gate, g_w_up, g_w_down)]
    new = [
        adamw(w.astype(jnp.float32), m, v, g)
        for w, m, v, g in zip((w_gate, w_up, w_down), (m_w_gate, m_w_up, m_w_down), (v_w_gate, v_w_up, v_w_down), gradients, strict=True)
    ]
    return tuple(one[which] for which in range(3) for one in new)
```

```python
import functools

import jax
import jax.numpy as jnp
from jax import lax
from jax.experimental import pallas as pl
from jax.experimental.pallas import tpu as pltpu
from jax.sharding import PartitionSpec as P

MESH = pl.DeviceIdType.MESH
CHIPS = 4
TILES = 35
HOP = 1
HOP2 = 1
LAG = 3
S_RAW, S_IN, S_OUT, S_ADAM, S_AG = 12, 8, 4, 3, 16
PIECE = 40


def tiles(x):
    *lead, r, c = x.shape
    return x.reshape(*lead, r // 8, 8, c // 128, 128).swapaxes(-3, -2).reshape(*lead, r * c // 128, 128)


def untiles(x, r, c):
    lead = x.shape[:-2]
    return x.reshape(*lead, r // 8, c // 128, 8, 128).swapaxes(-3, -2).reshape(*lead, r, c)


def kernel(
    per_layer, layers, *refs
):
    g, w, m, v = (refs[i : i + 3] for i in (0, 3, 6, 9))
    new_w, new_m, new_v = refs[12:15]
    own, sib, rin, lin, rout, lout, total, mi, vi, wi, mo, vo, wo = refs[15:28]
    own_sem, raw_s, raw_r, rs, rr, ls, lr, ld_sem, st_sem, own_s, fwd_s, ag_r, sib_s, sib_r = refs[28:]
    rows_per = TILES * 8
    n = len(g) * layers * per_layer
    d = lax.axis_index("dp")
    z, c = lax.div(d, 2), lax.rem(d, 2)
    right, left, twin = {"dp": lax.rem(d + 2, 8)}, {"dp": lax.rem(d + 6, 8)}, {"dp": z * 2 + 1 - c}
    far = jnp.maximum(z, CHIPS - 1 - z)

    def turn(o):
        return LAG + HOP * jnp.maximum(o, CHIPS - 1 - o)

    def place(i):
        which, rest = lax.div(i, layers * per_layer), lax.rem(i, layers * per_layer)
        layer, k = lax.div(rest, per_layer), lax.rem(rest, per_layer)
        return which, layer, pl.ds(pl.multiple_of(k * rows_per, 8), rows_per)

    def inside(i):
        return (i >= 0) & (i < n)

    def remote(src, dst, s, r, to):
        return pltpu.make_async_remote_copy(src, dst, s, r, device_id=to, device_id_type=MESH)

    def pieces(body):
        def one(p, _):
            body(pl.ds(pl.multiple_of(p * PIECE, 8), PIECE))
            return 0

        lax.fori_loop(0, rows_per // PIECE, one, 0)

    def f32(ref):
        return ref[...].astype(jnp.float32)

    barrier = pltpu.get_barrier_semaphore()

    @pl.when(z < CHIPS - 1)
    def _():
        pl.semaphore_signal(barrier, 1, device_id=right, device_id_type=MESH)

    @pl.when(z > 0)
    def _():
        pl.semaphore_signal(barrier, 1, device_id=left, device_id_type=MESH)

    pl.semaphore_signal(barrier, 1, device_id=twin, device_id_type=MESH)
    pl.semaphore_wait(barrier, 1 + (z > 0).astype(jnp.int32) + (z < CHIPS - 1).astype(jnp.int32))

    def raw(i):
        which, layer, rows = place(i)
        s = lax.rem(i, S_RAW)
        return which, [
            (
                pltpu.make_async_copy(one.at[layer, :, c, rows], own.at[s], own_sem.at[s]),
                remote(one.at[layer, :, 1 - c, rows], sib.at[s], raw_s.at[s], raw_r.at[s], twin),
            )
            for one in g
        ]

    def fetch(t):
        i = t

        @pl.when(inside(i))
        def _():
            which, copies = raw(i)

            @pl.when(i >= S_RAW)
            def _():
                copies[0][1].wait_send()

            for one, (mine, other) in enumerate(copies):

                @pl.when(which == one)
                def _():
                    other.start()
                    mine.start()

    def arrived(i):
        _, copies = raw(i)
        copies[0][0].wait()
        copies[0][1].wait_recv()

    def passing(t, rightward):
        if rightward:
            before, box, out, s_sem, r_sem, to = z, rin, rout, rs, rr, right
            many, has_in = CHIPS - 1 - z, z > 0
            first = z <= 1
            lane_of = lambda k: CHIPS - 1 - k
        else:
            before, box, out, s_sem, r_sem, to = CHIPS - 1 - z, lin, lout, ls, lr, left
            many, has_in = z, z < CHIPS - 1
            first = z > 1
            lane_of = lambda k: k
        i = t - LAG - HOP * before

        @pl.when(inside(i))
        def _():
            raw_slot, in_slot, out_slot = lax.rem(i, S_RAW), lax.rem(i, S_IN), lax.rem(i, S_OUT)

            def copy(o):
                return remote(out.at[out_slot, o], box.at[in_slot, o], s_sem.at[out_slot, o], r_sem.at[in_slot, o], to)

            @pl.when(first)
            def _():
                arrived(i)

            def lane(k, _):
                o = lane_of(k)

                @pl.when(i >= S_OUT)
                def _():
                    copy(o).wait_send()

                @pl.when(has_in)
                def _():
                    copy(o).wait_recv()

                    def add(rows):
                        so_far = f32(own.at[raw_slot, o, rows]) + f32(sib.at[raw_slot, o, rows])
                        out[out_slot, o, rows] = (so_far + f32(box.at[in_slot, o, rows])).astype(jnp.bfloat16)

                    pieces(add)

                @pl.when(jnp.logical_not(has_in))
                def _():
                    def add(rows):
                        so_far = f32(own.at[raw_slot, o, rows]) + f32(sib.at[raw_slot, o, rows])
                        out[out_slot, o, rows] = so_far.astype(jnp.bfloat16)

                    pieces(add)

                copy(o).start()
                return 0

            lax.fori_loop(0, many, lane, 0)

            @pl.when(has_in)
            def _():
                copy(z).wait_recv()

    def loads(i):
        which, layer, rows = place(i)
        s = lax.rem(i, S_ADAM)
        return which, [
            (
                pltpu.make_async_copy(m[one].at[layer, rows], mi.at[s], ld_sem.at[s, 0]),
                pltpu.make_async_copy(v[one].at[layer, rows], vi.at[s], ld_sem.at[s, 1]),
                pltpu.make_async_copy(w[one].at[layer, d, rows], wi.at[s], ld_sem.at[s, 2]),
            )
            for one in range(3)
        ]

    def fetch_state(t):
        i = t - turn(z) + S_ADAM - 1

        @pl.when(inside(i))
        def _():
            which, copies = loads(i)
            for one, each in enumerate(copies):

                @pl.when(which == one)
                def _():
                    for copy in each:
                        copy.start()

    def stores(i):
        which, layer, rows = place(i)
        s, a = lax.rem(i, S_ADAM), lax.rem(i, S_AG)
        there = new_w.at[which, layer, d, rows]
        local = [
            pltpu.make_async_copy(mo.at[s], new_m.at[which, layer, rows], st_sem.at[s, 0]),
            pltpu.make_async_copy(vo.at[s], new_v.at[which, layer, rows], st_sem.at[s, 1]),
            pltpu.make_async_copy(wo.at[s], there, st_sem.at[s, 2]),
        ]
        to_right = remote(wo.at[s], there, own_s.at[s, 0], ag_r.at[a, z], right)
        to_left = remote(wo.at[s], there, own_s.at[s, 1], ag_r.at[a, z], left)
        to_twin = remote(wo.at[s], there, own_s.at[s, 2], sib_r.at[a, z], twin)
        return local, to_right, to_left, to_twin

    def stored(i):
        local, to_right, to_left, to_twin = stores(i)
        for copy in local:
            copy.wait()
        to_twin.wait_send()

        @pl.when(z < CHIPS - 1)
        def _():
            to_right.wait_send()

        @pl.when(z > 0)
        def _():
            to_left.wait_send()

    def adam(t):
        i = t - turn(z)

        @pl.when(inside(i))
        def _():
            raw_slot, in_slot, s = lax.rem(i, S_RAW), lax.rem(i, S_IN), lax.rem(i, S_ADAM)
            _, copies = loads(i)
            for copy in copies[0]:
                copy.wait()

            @pl.when(i >= S_ADAM)
            def _():
                stored(i - S_ADAM)

            def begin(rows):
                total[rows] = f32(own.at[raw_slot, z, rows]) + f32(sib.at[raw_slot, z, rows])

            pieces(begin)

            @pl.when(z > 0)
            def _():
                def add(rows):
                    total[rows] += f32(rin.at[in_slot, z, rows])

                pieces(add)

            @pl.when(z < CHIPS - 1)
            def _():
                def add(rows):
                    total[rows] += f32(lin.at[in_slot, z, rows])

                pieces(add)

            def step(rows):
                grad = total[rows].astype(jnp.bfloat16).astype(jnp.float32)
                m1 = 0.9 * mi[s, rows] + 0.1 * grad
                v1 = 0.95 * vi[s, rows] + 0.05 * grad * grad
                w0 = f32(wi.at[s, rows])
                mo[s, rows] = m1
                vo[s, rows] = v1
                wo[s, rows] = (w0 - 0.02 * (m1 * lax.rsqrt(v1 + 1e-8) + 0.1 * w0)).astype(jnp.bfloat16)

            pieces(step)
            local, to_right, to_left, to_twin = stores(i)

            @pl.when(z < CHIPS - 1)
            def _():
                to_right.start()

            @pl.when(z > 0)
            def _():
                to_left.start()

            to_twin.start()
            for copy in local:
                copy.start()

    def forwards(i, o, to):
        which, layer, rows = place(i)
        a = lax.rem(i, S_AG)
        there = new_w.at[which, layer, o * 2 + c, rows]
        return remote(there, there, fwd_s.at[a, o], ag_r.at[a, o], to), remote(there, there, sib_s.at[a, o], sib_r.at[a, o], twin)

    def sent(i, o, to, on):
        ahead, across = forwards(i, o, to)

        @pl.when(on)
        def _():
            ahead.wait_send()

        across.wait_send()

    def gathering(t, rightward):
        many, to, on = (z, right, z < CHIPS - 1) if rightward else (CHIPS - 1 - z, left, z > 0)

        def lane(k, _):
            o = z - 1 - k if rightward else z + 1 + k
            i = t - turn(o) - HOP2 * (k + 1)

            @pl.when(inside(i))
            def _():
                @pl.when(i >= S_AG)
                def _():
                    sent(i - S_AG, o, to, on)

                ahead, across = forwards(i, o, to)
                ahead.wait_recv()

                @pl.when(on)
                def _():
                    ahead.start()

                across.start()

            return 0

        lax.fori_loop(0, many, lane, 0)

    def crossing(t):
        def lane(o, _):
            i = t - turn(o) - HOP2 * jnp.abs(z - o) - 2

            @pl.when(inside(i))
            def _():
                forwards(i, o, right)[1].wait_recv()

            return 0

        lax.fori_loop(0, CHIPS, lane, 0)

    def step(t, _):
        passing(t, True)
        passing(t, False)
        adam(t)
        gathering(t, True)
        gathering(t, False)
        fetch(t)
        fetch_state(t)
        crossing(t)
        return 0

    lax.fori_loop(0, n + LAG + (HOP + HOP2) * (CHIPS - 1) + 3, step, 0)

    def raw_left(k, _):
        raw(n - S_RAW + k)[1][0][1].wait_send()
        return 0

    lax.fori_loop(0, S_RAW, raw_left, 0)

    def pass_left(k, _):
        i = n - S_OUT + k
        s, e = lax.rem(i, S_OUT), lax.rem(i, S_IN)

        def to_right(o, _):
            remote(rout.at[s, o], rin.at[e, o], rs.at[s, o], rr.at[e, o], right).wait_send()
            return 0

        def to_left(o, _):
            remote(lout.at[s, o], lin.at[e, o], ls.at[s, o], lr.at[e, o], left).wait_send()
            return 0

        lax.fori_loop(z + 1, CHIPS, to_right, 0)
        lax.fori_loop(0, z, to_left, 0)
        return 0

    lax.fori_loop(0, S_OUT, pass_left, 0)

    def stores_left(k, _):
        stored(n - S_ADAM + k)
        return 0

    lax.fori_loop(0, S_ADAM, stores_left, 0)

    def gather_left(k, _):
        i = n - S_AG + k

        def of_left(o, _):
            sent(i, o, right, z < CHIPS - 1)
            return 0

        def of_right(o, _):
            sent(i, o, left, z > 0)
            return 0

        lax.fori_loop(0, z, of_left, 0)
        lax.fori_loop(z + 1, CHIPS, of_right, 0)
        return 0

    lax.fori_loop(0, S_AG, gather_left, 0)


def solution(mesh):
    bf16, f32 = jnp.bfloat16, jnp.float32

    def step(*arrays):
        terms, weights, m, v = (arrays[i : i + 3] for i in (0, 3, 6, 9))
        layers = weights[0].shape[0]
        block = weights[0].shape[1] * weights[0].shape[2] // (2 * CHIPS * 128)
        rows = TILES * 8
        args = [tiles(t[0]).reshape(layers, CHIPS, 2, block, 128) for t in terms]
        args += [tiles(w).reshape(layers, 2 * CHIPS, block, 128) for w in weights]
        args += [tiles(x) for x in (*m, *v)]
        dma = pltpu.SemaphoreType.DMA
        new_w, new_m, new_v = pl.pallas_call(
            functools.partial(kernel, block // rows, layers),
            out_shape=[
                jax.ShapeDtypeStruct((3, layers, 2 * CHIPS, block, 128), bf16),
                jax.ShapeDtypeStruct((3, layers, block, 128), f32),
                jax.ShapeDtypeStruct((3, layers, block, 128), f32),
            ],
            in_specs=[pl.BlockSpec(memory_space=pl.ANY)] * 12,
            out_specs=[pl.BlockSpec(memory_space=pl.ANY)] * 3,
            scratch_shapes=[
                pltpu.VMEM((S_RAW, CHIPS, rows, 128), bf16),
                pltpu.VMEM((S_RAW, CHIPS, rows, 128), bf16),
                pltpu.VMEM((S_IN, CHIPS, rows, 128), bf16),
                pltpu.VMEM((S_IN, CHIPS, rows, 128), bf16),
                pltpu.VMEM((S_OUT, CHIPS, rows, 128), bf16),
                pltpu.VMEM((S_OUT, CHIPS, rows, 128), bf16),
                pltpu.VMEM((rows, 128), f32),
                pltpu.VMEM((S_ADAM, rows, 128), f32),
                pltpu.VMEM((S_ADAM, rows, 128), f32),
                pltpu.VMEM((S_ADAM, rows, 128), bf16),
                pltpu.VMEM((S_ADAM, rows, 128), f32),
                pltpu.VMEM((S_ADAM, rows, 128), f32),
                pltpu.VMEM((S_ADAM, rows, 128), bf16),
                dma((S_RAW,)),
                dma((S_RAW,)),
                dma((S_RAW,)),
                dma((S_OUT, CHIPS)),
                dma((S_IN, CHIPS)),
                dma((S_OUT, CHIPS)),
                dma((S_IN, CHIPS)),
                dma((S_ADAM, 3)),
                dma((S_ADAM, 3)),
                dma((S_ADAM, 3)),
                dma((S_AG, CHIPS)),
                dma((S_AG, CHIPS)),
                dma((S_AG, CHIPS)),
                dma((S_AG, CHIPS)),
            ],
            compiler_params=pltpu.CompilerParams(collective_id=0, has_side_effects=True),
        )(*args)
        outs = [untiles(new_w[k].reshape(layers, -1, 128), *weights[k].shape[1:]) for k in range(3)]
        for new, old in ((new_m, m), (new_v, v)):
            outs += [untiles(new[k], *old[k].shape[1:]) for k in range(3)]
        return tuple(outs)

    all_of, cut = P(None, None, None), P(None, "dp", None)
    return jax.shard_map(
        step,
        mesh=mesh,
        in_specs=(P(("rep", "dp"), None, None, None),) * 3 + (all_of,) * 3 + (cut,) * 6,
        out_specs=(P("rep", None, None),) * 3 + (P("rep", "dp", None),) * 6,
        check_vma=False,
    )
```

```python
import functools

import jax
import jax.numpy as jnp
from jax import lax
from jax.experimental import pallas as pl
from jax.experimental.pallas import tpu as pltpu
from jax.sharding import PartitionSpec as P

MESH = pl.DeviceIdType.MESH
CHIPS = 4
TILES = 28
HOP = 1
HOP2 = 1
LAG = 2
S_RAW, S_IN, S_OUT, S_ADAM, S_AG = 10, 6, 3, 3, 16
ROOM = 9472 * 1024
SPANS, S_COPY = 32, 12
PIECE = 32


def tiles(x):
    *lead, r, c = x.shape
    return x.reshape(*lead, r // 8, 8, c // 128, 128).swapaxes(-3, -2).reshape(*lead, r * c // 128, 128)


def untiles(x, r, c):
    lead = x.shape[:-2]
    return x.reshape(*lead, r // 8, c // 128, 8, 128).swapaxes(-3, -2).reshape(*lead, r, c)


def kernel(
    per_layer, layers, *refs
):
    g, w, m, v = (refs[i : i + 3] for i in (0, 3, 6, 9))
    new_w, last_w, state = refs[12:15]
    new_m, new_v = state.at[0], state.at[1]
    own, sib, rin, lin, rout, lout, total, wi, wo = refs[15:24]
    own_sem, raw_s, raw_r, rs, rr, ls, lr, ld_sem, st_sem, own_s, fwd_s, ag_r, sib_s, sib_r = refs[24:]
    rows_per = TILES * 8
    n = len(g) * layers * per_layer
    d = lax.axis_index("dp")
    z, c = lax.div(d, 2), lax.rem(d, 2)
    right, left, twin = {"dp": lax.rem(d + 2, 8)}, {"dp": lax.rem(d + 6, 8)}, {"dp": z * 2 + 1 - c}
    far = jnp.maximum(z, CHIPS - 1 - z)

    def turn(o):
        return LAG + HOP * jnp.maximum(o, CHIPS - 1 - o)

    def place(i):
        which, rest = lax.div(i, layers * per_layer), lax.rem(i, layers * per_layer)
        layer, k = lax.div(rest, per_layer), lax.rem(rest, per_layer)
        return which, layer, pl.ds(pl.multiple_of(k * rows_per, 8), rows_per)

    def spots(i, owner):
        which, layer, rows = place(i)
        late = i >= n - per_layer
        return (jnp.logical_not(late), new_w.at[which, layer, owner, rows]), (late, last_w.at[owner, rows])

    def inside(i):
        return (i >= 0) & (i < n)

    def remote(src, dst, s, r, to):
        return pltpu.make_async_remote_copy(src, dst, s, r, device_id=to, device_id_type=MESH)

    def pieces(body):
        def one(p, _):
            body(pl.ds(pl.multiple_of(p * PIECE, 8), PIECE))
            return 0

        lax.fori_loop(0, rows_per // PIECE, one, 0)

    def f32(ref):
        return ref[...].astype(jnp.float32)

    barrier = pltpu.get_barrier_semaphore()

    @pl.when(z < CHIPS - 1)
    def _():
        pl.semaphore_signal(barrier, 1, device_id=right, device_id_type=MESH)

    @pl.when(z > 0)
    def _():
        pl.semaphore_signal(barrier, 1, device_id=left, device_id_type=MESH)

    pl.semaphore_signal(barrier, 1, device_id=twin, device_id_type=MESH)
    pl.semaphore_wait(barrier, 1 + (z > 0).astype(jnp.int32) + (z < CHIPS - 1).astype(jnp.int32))

    def raw(i):
        which, layer, rows = place(i)
        s = lax.rem(i, S_RAW)
        return which, [
            (
                pltpu.make_async_copy(one.at[layer, :, c, rows], own.at[s], own_sem.at[s]),
                remote(one.at[layer, :, 1 - c, rows], sib.at[s], raw_s.at[s], raw_r.at[s], twin),
            )
            for one in g
        ]

    def fetch(t):
        i = t

        @pl.when(inside(i))
        def _():
            which, copies = raw(i)

            @pl.when(i >= S_RAW)
            def _():
                copies[0][1].wait_send()

            for one, (mine, other) in enumerate(copies):

                @pl.when(which == one)
                def _():
                    other.start()
                    mine.start()

    def arrived(i):
        _, copies = raw(i)
        copies[0][0].wait()
        copies[0][1].wait_recv()

    def passing(t, rightward):
        if rightward:
            before, box, out, s_sem, r_sem, to = z, rin, rout, rs, rr, right
            many, has_in = CHIPS - 1 - z, z > 0
            first = z <= 1
            lane_of = lambda k: CHIPS - 1 - k
        else:
            before, box, out, s_sem, r_sem, to = CHIPS - 1 - z, lin, lout, ls, lr, left
            many, has_in = z, z < CHIPS - 1
            first = z > 1
            lane_of = lambda k: k
        i = t - LAG - HOP * before

        @pl.when(inside(i))
        def _():
            raw_slot, in_slot, out_slot = lax.rem(i, S_RAW), lax.rem(i, S_IN), lax.rem(i, S_OUT)

            def copy(o):
                return remote(out.at[out_slot, o], box.at[in_slot, o], s_sem.at[out_slot, o], r_sem.at[in_slot, o], to)

            @pl.when(first)
            def _():
                arrived(i)

            def lane(k, _):
                o = lane_of(k)

                @pl.when(i >= S_OUT)
                def _():
                    copy(o).wait_send()

                @pl.when(has_in)
                def _():
                    copy(o).wait_recv()

                    def add(rows):
                        so_far = f32(own.at[raw_slot, o, rows]) + f32(sib.at[raw_slot, o, rows])
                        out[out_slot, o, rows] = (so_far + f32(box.at[in_slot, o, rows])).astype(jnp.bfloat16)

                    pieces(add)

                @pl.when(jnp.logical_not(has_in))
                def _():
                    def add(rows):
                        so_far = f32(own.at[raw_slot, o, rows]) + f32(sib.at[raw_slot, o, rows])
                        out[out_slot, o, rows] = so_far.astype(jnp.bfloat16)

                    pieces(add)

                copy(o).start()
                return 0

            lax.fori_loop(0, many, lane, 0)

            @pl.when(has_in)
            def _():
                copy(z).wait_recv()

    def loads(i):
        which, layer, rows = place(i)
        s = lax.rem(i, S_ADAM)
        return which, [
            (
                pltpu.make_async_copy(m[one].at[layer, rows], new_m.at[one, layer, rows], ld_sem.at[s, 0]),
                pltpu.make_async_copy(v[one].at[layer, rows], new_v.at[one, layer, rows], ld_sem.at[s, 1]),
                pltpu.make_async_copy(w[one].at[layer, d, rows], wi.at[s], ld_sem.at[s, 2]),
            )
            for one in range(3)
        ]

    def fetch_state(t):
        i = t - turn(z) + S_ADAM - 1

        @pl.when(inside(i))
        def _():
            which, copies = loads(i)
            for one, each in enumerate(copies):

                @pl.when(which == one)
                def _():
                    for copy in each:
                        copy.start()

    def stores(i, there):
        s, a = lax.rem(i, S_ADAM), lax.rem(i, S_AG)
        local = pltpu.make_async_copy(wo.at[s], there, st_sem.at[s])
        to_right = remote(wo.at[s], there, own_s.at[s, 0], ag_r.at[a, z], right)
        to_left = remote(wo.at[s], there, own_s.at[s, 1], ag_r.at[a, z], left)
        to_twin = remote(wo.at[s], there, own_s.at[s, 2], sib_r.at[a, z], twin)
        return local, to_right, to_left, to_twin

    def stored(i):
        (in_hbm, there), _ = spots(i, d)
        local, to_right, to_left, to_twin = stores(i, there)

        @pl.when(in_hbm)
        def _():
            local.wait()

        to_twin.wait_send()

        @pl.when(z < CHIPS - 1)
        def _():
            to_right.wait_send()

        @pl.when(z > 0)
        def _():
            to_left.wait_send()

    def adam(t):
        i = t - turn(z)

        @pl.when(inside(i))
        def _():
            raw_slot, in_slot, s = lax.rem(i, S_RAW), lax.rem(i, S_IN), lax.rem(i, S_ADAM)
            _, copies = loads(i)
            for copy in copies[0]:
                copy.wait()

            @pl.when(i >= S_ADAM)
            def _():
                stored(i - S_ADAM)

            def begin(rows):
                total[rows] = f32(own.at[raw_slot, z, rows]) + f32(sib.at[raw_slot, z, rows])

            pieces(begin)

            @pl.when(z > 0)
            def _():
                def add(rows):
                    total[rows] += f32(rin.at[in_slot, z, rows])

                pieces(add)

            @pl.when(z < CHIPS - 1)
            def _():
                def add(rows):
                    total[rows] += f32(lin.at[in_slot, z, rows])

                pieces(add)

            which, layer, base = place(i)

            def step(rows):
                to = pl.ds(pl.multiple_of(base.start + rows.start, 8), PIECE)
                grad = total[rows].astype(jnp.bfloat16).astype(jnp.float32)
                m1 = 0.9 * new_m[which, layer, to] + 0.1 * grad
                v1 = 0.95 * new_v[which, layer, to] + 0.05 * grad * grad
                w0 = f32(wi.at[s, rows])
                new_m[which, layer, to] = m1
                new_v[which, layer, to] = v1
                wo[s, rows] = (w0 - 0.02 * (m1 * lax.rsqrt(v1 + 1e-8) + 0.1 * w0)).astype(jnp.bfloat16)

            pieces(step)

            @pl.when(i >= n - per_layer)
            def _():
                def keep(rows):
                    last_w[d, pl.ds(pl.multiple_of(base.start + rows.start, 8), PIECE)] = wo[s, rows]

                pieces(keep)

            for here, there in spots(i, d):

                @pl.when(here)
                def _(there=there):
                    local, to_right, to_left, to_twin = stores(i, there)

                    @pl.when(z < CHIPS - 1)
                    def _():
                        to_right.start()

                    @pl.when(z > 0)
                    def _():
                        to_left.start()

                    to_twin.start()
                    if there.memory_space != pltpu.VMEM:
                        local.start()

    def forwards(i, o, to, there):
        a = lax.rem(i, S_AG)
        return remote(there, there, fwd_s.at[a, o], ag_r.at[a, o], to), remote(there, there, sib_s.at[a, o], sib_r.at[a, o], twin)

    def sent(i, o, to, on):
        ahead, across = forwards(i, o, to, spots(i, 0)[0][1])

        @pl.when(on)
        def _():
            ahead.wait_send()

        across.wait_send()

    def gathering(t, rightward):
        many, to, on = (z, right, z < CHIPS - 1) if rightward else (CHIPS - 1 - z, left, z > 0)

        def lane(k, _):
            o = z - 1 - k if rightward else z + 1 + k
            i = t - turn(o) - HOP2 * (k + 1)

            @pl.when(inside(i))
            def _():
                @pl.when(i >= S_AG)
                def _():
                    sent(i - S_AG, o, to, on)

                forwards(i, o, to, spots(i, 0)[0][1])[0].wait_recv()
                for here, there in spots(i, o * 2 + c):

                    @pl.when(here)
                    def _(there=there):
                        ahead, across = forwards(i, o, to, there)

                        @pl.when(on)
                        def _():
                            ahead.start()

                        across.start()

            return 0

        lax.fori_loop(0, many, lane, 0)

    def crossing(t):
        def lane(o, _):
            i = t - turn(o) - HOP2 * jnp.abs(z - o) - 2

            @pl.when(inside(i))
            def _():
                forwards(i, o, right, spots(i, 0)[0][1])[1].wait_recv()

            return 0

        lax.fori_loop(0, CHIPS, lane, 0)

    def step(t, _):
        passing(t, True)
        passing(t, False)
        adam(t)
        gathering(t, True)
        gathering(t, False)
        fetch(t)
        fetch_state(t)
        crossing(t)
        return 0

    lax.fori_loop(0, n + LAG + (HOP + HOP2) * (CHIPS - 1) + 3, step, 0)

    def raw_left(k, _):
        raw(n - S_RAW + k)[1][0][1].wait_send()
        return 0

    lax.fori_loop(0, S_RAW, raw_left, 0)

    def pass_left(k, _):
        i = n - S_OUT + k
        s, e = lax.rem(i, S_OUT), lax.rem(i, S_IN)

        def to_right(o, _):
            remote(rout.at[s, o], rin.at[e, o], rs.at[s, o], rr.at[e, o], right).wait_send()
            return 0

        def to_left(o, _):
            remote(lout.at[s, o], lin.at[e, o], ls.at[s, o], lr.at[e, o], left).wait_send()
            return 0

        lax.fori_loop(z + 1, CHIPS, to_right, 0)
        lax.fori_loop(0, z, to_left, 0)
        return 0

    lax.fori_loop(0, S_OUT, pass_left, 0)

    def stores_left(k, _):
        stored(n - S_ADAM + k)
        return 0

    lax.fori_loop(0, S_ADAM, stores_left, 0)

    def gather_left(k, _):
        i = n - S_AG + k

        def of_left(o, _):
            sent(i, o, right, z < CHIPS - 1)
            return 0

        def of_right(o, _):
            sent(i, o, left, z > 0)
            return 0

        lax.fori_loop(0, z, of_left, 0)
        lax.fori_loop(z + 1, CHIPS, of_right, 0)
        return 0

    lax.fori_loop(0, S_AG, gather_left, 0)


def finish(new_w, last_w, state, *refs):
    outs, (held, in_sem, out_sem, sem) = refs[:9], refs[9:]
    straight = [pltpu.make_async_copy(last_w, outs[2].at[outs[2].shape[0] - 1], sem.at[6])]
    for k in range(6):
        straight.append(pltpu.make_async_copy(state.at[k // 3, k % 3], outs[3 + k], sem.at[k]))
    span = held.shape[1]
    per = new_w.shape[2] // span

    def load(j):
        k, layer, p = j // SPANS, j % SPANS // per, j % per
        return pltpu.make_async_copy(new_w.at[k, layer, pl.ds(p * span, span)], held.at[j % S_COPY], in_sem.at[j % S_COPY])

    def store(j):
        k, layer, p = j // SPANS, j % SPANS // per, j % per
        return pltpu.make_async_copy(held.at[j % S_COPY], outs[k].at[layer, pl.ds(p * span, span)], out_sem.at[j % S_COPY])

    n = 3 * SPANS - per
    ahead = S_COPY - 3
    for j in range(ahead):
        load(j).start()
    for copy in straight:
        copy.start()
    for j in range(n):
        load(j).wait()
        store(j).start()
        if j + ahead < n:
            if j + ahead >= S_COPY:
                store(j + ahead - S_COPY).wait()
            load(j + ahead).start()
    for j in range(n - S_COPY, n):
        store(j).wait()
    for copy in straight:
        copy.wait()


def solution(mesh):
    bf16, f32 = jnp.bfloat16, jnp.float32

    def step(*arrays):
        terms, weights, m, v = (arrays[i : i + 3] for i in (0, 3, 6, 9))
        layers = weights[0].shape[0]
        block = weights[0].shape[1] * weights[0].shape[2] // (2 * CHIPS * 128)
        rows = TILES * 8
        args = [tiles(t[0]).reshape(layers, CHIPS, 2, block, 128) for t in terms]
        args += [tiles(w).reshape(layers, 2 * CHIPS, block, 128) for w in weights]
        args += [tiles(x) for x in (*m, *v)]
        dma = pltpu.SemaphoreType.DMA
        new_w, last_w, state = pl.pallas_call(
            functools.partial(kernel, block // rows, layers),
            out_shape=[
                jax.ShapeDtypeStruct((3, layers, 2 * CHIPS, block, 128), bf16),
                pltpu.VMEM((2 * CHIPS, block, 128), bf16),
                pltpu.VMEM((2, 3, layers, block, 128), f32),
            ],
            in_specs=[pl.BlockSpec(memory_space=pltpu.HBM)] * 12,
            out_specs=[pl.BlockSpec(memory_space=pltpu.HBM)] + [pl.BlockSpec(memory_space=pltpu.VMEM)] * 2,
            scratch_shapes=[
                pltpu.VMEM((S_RAW, CHIPS, rows, 128), bf16),
                pltpu.VMEM((S_RAW, CHIPS, rows, 128), bf16),
                pltpu.VMEM((S_IN, CHIPS, rows, 128), bf16),
                pltpu.VMEM((S_IN, CHIPS, rows, 128), bf16),
                pltpu.VMEM((S_OUT, CHIPS, rows, 128), bf16),
                pltpu.VMEM((S_OUT, CHIPS, rows, 128), bf16),
                pltpu.VMEM((rows, 128), f32),
                pltpu.VMEM((S_ADAM, rows, 128), bf16),
                pltpu.VMEM((S_ADAM, rows, 128), bf16),
                dma((S_RAW,)),
                dma((S_RAW,)),
                dma((S_RAW,)),
                dma((S_OUT, CHIPS)),
                dma((S_IN, CHIPS)),
                dma((S_OUT, CHIPS)),
                dma((S_IN, CHIPS)),
                dma((S_ADAM, 3)),
                dma((S_ADAM,)),
                dma((S_ADAM, 3)),
                dma((S_AG, CHIPS)),
                dma((S_AG, CHIPS)),
                dma((S_AG, CHIPS)),
                dma((S_AG, CHIPS)),
            ],
            compiler_params=pltpu.CompilerParams(collective_id=0, has_side_effects=True, vmem_limit_bytes=ROOM),
        )(*args)
        flat = [jax.ShapeDtypeStruct((layers, 2 * CHIPS * block, 128), bf16)] * 3 + [jax.ShapeDtypeStruct((layers, block, 128), f32)] * 6
        span = layers * 2 * CHIPS * block // SPANS
        outs = pl.pallas_call(
            finish,
            out_shape=flat,
            in_specs=[pl.BlockSpec(memory_space=pltpu.HBM)] + [pl.BlockSpec(memory_space=pltpu.VMEM)] * 2,
            out_specs=[pl.BlockSpec(memory_space=pltpu.HBM)] * 9,
            scratch_shapes=[pltpu.VMEM((S_COPY, span, 128), bf16), dma((S_COPY,)), dma((S_COPY,)), dma((7,))],
            compiler_params=pltpu.CompilerParams(vmem_limit_bytes=ROOM),
        )(new_w.reshape(3, layers, 2 * CHIPS * block, 128), last_w.reshape(2 * CHIPS * block, 128), state)
        outs = [untiles(o, *old.shape[1:]) for o, old in zip(outs, (*weights, *m, *v), strict=True)]
        return tuple(outs)

    all_of, cut = P(None, None, None), P(None, "dp", None)
    return jax.shard_map(
        step,
        mesh=mesh,
        in_specs=(P(("rep", "dp"), None, None, None),) * 3 + (all_of,) * 3 + (cut,) * 6,
        out_specs=(P("rep", None, None),) * 3 + (P("rep", "dp", None),) * 6,
        check_vma=False,
    )
```

```python
import functools

import jax
import jax.numpy as jnp
from jax import lax
from jax.experimental import pallas as pl
from jax.experimental.pallas import tpu as pltpu
from jax.sharding import PartitionSpec as P

MESH = pl.DeviceIdType.MESH
CHIPS = 4
TILES = 28
HOP = 1
HOP2 = 1
LAG = 2
S_RAW, S_IN, S_OUT, S_ADAM, S_AG = 10, 6, 3, 3, 16
LATE = 10
HELD = 15
ROOM = 9472 * 1024
SPAN, S_COPY = 2800, 12
MOST_COST = 10**11
PIECE = 32


def tiles(x):
    *lead, r, c = x.shape
    return x.reshape(*lead, r // 8, 8, c // 128, 128).swapaxes(-3, -2).reshape(*lead, r * c // 128, 128)


def untiles(x, r, c):
    lead = x.shape[:-2]
    return x.reshape(*lead, r // 8, c // 128, 8, 128).swapaxes(-3, -2).reshape(*lead, r, c)


def kernel(
    per_layer, layers, *refs
):
    g, w, m, v = (refs[i : i + 3] for i in (0, 3, 6, 9))
    new_w, last_w, late_w, late_twin, state = refs[12:17]
    new_m, new_v = state.at[0], state.at[1]
    own, sib, rin, lin, rout, lout, total, wi, wo = refs[17:26]
    own_sem, raw_s, raw_r, rs, rr, ls, lr, ld_sem, st_sem, own_s, fwd_s, ag_r, sib_s, sib_r = refs[26:]
    rows_per = TILES * 8
    n = len(g) * layers * per_layer
    early = n - LATE
    d = lax.axis_index("dp")
    z, c = lax.div(d, 2), lax.rem(d, 2)
    right, left, twin = {"dp": lax.rem(d + 2, 8)}, {"dp": lax.rem(d + 6, 8)}, {"dp": z * 2 + 1 - c}
    far = jnp.maximum(z, CHIPS - 1 - z)

    def turn(o):
        return LAG + HOP * jnp.maximum(o, CHIPS - 1 - o)

    def place(i):
        which, rest = lax.div(i, layers * per_layer), lax.rem(i, layers * per_layer)
        layer, k = lax.div(rest, per_layer), lax.rem(rest, per_layer)
        return which, layer, pl.ds(pl.multiple_of(k * rows_per, 8), rows_per)

    def spots(i, owner):
        which, layer, rows = place(i)
        at = pl.ds(pl.multiple_of((i - (early - HELD)) * rows_per, 8), rows_per)
        return (i < early - HELD, new_w.at[which, layer, owner, rows]), (i >= early - HELD, last_w.at[owner, at])

    def inside(i):
        return (i >= 0) & (i < n)

    def remote(src, dst, s, r, to):
        return pltpu.make_async_remote_copy(src, dst, s, r, device_id=to, device_id_type=MESH)

    def pieces(body):
        def one(p, _):
            body(pl.ds(pl.multiple_of(p * PIECE, 8), PIECE))
            return 0

        lax.fori_loop(0, rows_per // PIECE, one, 0)

    def f32(ref):
        return ref[...].astype(jnp.float32)

    barrier = pltpu.get_barrier_semaphore()

    @pl.when(z < CHIPS - 1)
    def _():
        pl.semaphore_signal(barrier, 1, device_id=right, device_id_type=MESH)

    @pl.when(z > 0)
    def _():
        pl.semaphore_signal(barrier, 1, device_id=left, device_id_type=MESH)

    pl.semaphore_signal(barrier, 1, device_id=twin, device_id_type=MESH)
    pl.semaphore_wait(barrier, 1 + (z > 0).astype(jnp.int32) + (z < CHIPS - 1).astype(jnp.int32))

    def raw(i):
        which, layer, rows = place(i)
        s = lax.rem(i, S_RAW)
        return which, [
            (
                pltpu.make_async_copy(one.at[layer, :, c, rows], own.at[s], own_sem.at[s]),
                remote(one.at[layer, :, 1 - c, rows], sib.at[s], raw_s.at[s], raw_r.at[s], twin),
            )
            for one in g
        ]

    def fetch(t):
        i = t

        @pl.when(inside(i))
        def _():
            which, copies = raw(i)

            @pl.when(i >= S_RAW)
            def _():
                copies[0][1].wait_send()

            for one, (mine, other) in enumerate(copies):

                @pl.when(which == one)
                def _():
                    other.start()
                    mine.start()

    def arrived(i):
        _, copies = raw(i)
        copies[0][0].wait()
        copies[0][1].wait_recv()

    def passing(t, rightward):
        if rightward:
            before, box, out, s_sem, r_sem, to = z, rin, rout, rs, rr, right
            many, has_in = CHIPS - 1 - z, z > 0
            first = z <= 1
            lane_of = lambda k: CHIPS - 1 - k
        else:
            before, box, out, s_sem, r_sem, to = CHIPS - 1 - z, lin, lout, ls, lr, left
            many, has_in = z, z < CHIPS - 1
            first = z > 1
            lane_of = lambda k: k
        i = t - LAG - HOP * before

        @pl.when(inside(i))
        def _():
            raw_slot, in_slot, out_slot = lax.rem(i, S_RAW), lax.rem(i, S_IN), lax.rem(i, S_OUT)

            def copy(o):
                return remote(out.at[out_slot, o], box.at[in_slot, o], s_sem.at[out_slot, o], r_sem.at[in_slot, o], to)

            @pl.when(first)
            def _():
                arrived(i)

            def lane(k, _):
                o = lane_of(k)

                @pl.when(i >= S_OUT)
                def _():
                    copy(o).wait_send()

                @pl.when(has_in)
                def _():
                    copy(o).wait_recv()

                    def add(rows):
                        so_far = f32(own.at[raw_slot, o, rows]) + f32(sib.at[raw_slot, o, rows])
                        out[out_slot, o, rows] = (so_far + f32(box.at[in_slot, o, rows])).astype(jnp.bfloat16)

                    pieces(add)

                @pl.when(jnp.logical_not(has_in))
                def _():
                    def add(rows):
                        so_far = f32(own.at[raw_slot, o, rows]) + f32(sib.at[raw_slot, o, rows])
                        out[out_slot, o, rows] = so_far.astype(jnp.bfloat16)

                    pieces(add)

                copy(o).start()
                return 0

            lax.fori_loop(0, many, lane, 0)

            @pl.when(has_in)
            def _():
                copy(z).wait_recv()

    def loads(i):
        which, layer, rows = place(i)
        s = lax.rem(i, S_ADAM)
        return which, [
            (
                pltpu.make_async_copy(m[one].at[layer, rows], new_m.at[one, layer, rows], ld_sem.at[s, 0]),
                pltpu.make_async_copy(v[one].at[layer, rows], new_v.at[one, layer, rows], ld_sem.at[s, 1]),
                pltpu.make_async_copy(w[one].at[layer, d, rows], wi.at[s], ld_sem.at[s, 2]),
            )
            for one in range(3)
        ]

    def fetch_state(t):
        i = t - turn(z) + S_ADAM - 1

        @pl.when(inside(i))
        def _():
            which, copies = loads(i)
            for one, each in enumerate(copies):

                @pl.when(which == one)
                def _():
                    for copy in each:
                        copy.start()

    def stores(i, there):
        s, a = lax.rem(i, S_ADAM), lax.rem(i, S_AG)
        local = pltpu.make_async_copy(wo.at[s], there, st_sem.at[s])
        to_right = remote(wo.at[s], there, own_s.at[s, 0], ag_r.at[a, z], right)
        to_left = remote(wo.at[s], there, own_s.at[s, 1], ag_r.at[a, z], left)
        to_twin = remote(wo.at[s], there, own_s.at[s, 2], sib_r.at[a, z], twin)
        return local, to_right, to_left, to_twin

    def stored(i):
        (in_hbm, there), _ = spots(i, d)
        local, to_right, to_left, to_twin = stores(i, there)

        @pl.when(in_hbm | (i >= early))
        def _():
            local.wait()

        to_twin.wait_send()

        @pl.when((i < early) & (z < CHIPS - 1))
        def _():
            to_right.wait_send()

        @pl.when((i < early) & (z > 0))
        def _():
            to_left.wait_send()

    def adam(t):
        i = t - turn(z)

        @pl.when(inside(i))
        def _():
            raw_slot, in_slot, s = lax.rem(i, S_RAW), lax.rem(i, S_IN), lax.rem(i, S_ADAM)
            _, copies = loads(i)
            for copy in copies[0]:
                copy.wait()

            @pl.when(i >= S_ADAM)
            def _():
                stored(i - S_ADAM)

            def begin(rows):
                total[rows] = f32(own.at[raw_slot, z, rows]) + f32(sib.at[raw_slot, z, rows])

            pieces(begin)

            @pl.when(z > 0)
            def _():
                def add(rows):
                    total[rows] += f32(rin.at[in_slot, z, rows])

                pieces(add)

            @pl.when(z < CHIPS - 1)
            def _():
                def add(rows):
                    total[rows] += f32(lin.at[in_slot, z, rows])

                pieces(add)

            which, layer, base = place(i)

            def step(rows):
                to = pl.ds(pl.multiple_of(base.start + rows.start, 8), PIECE)
                grad = total[rows].astype(jnp.bfloat16).astype(jnp.float32)
                m1 = 0.9 * new_m[which, layer, to] + 0.1 * grad
                v1 = 0.95 * new_v[which, layer, to] + 0.05 * grad * grad
                w0 = f32(wi.at[s, rows])
                new_m[which, layer, to] = m1
                new_v[which, layer, to] = v1
                wo[s, rows] = (w0 - 0.02 * (m1 * lax.rsqrt(v1 + 1e-8) + 0.1 * w0)).astype(jnp.bfloat16)

            pieces(step)

            @pl.when((i >= early - HELD) & (i < early))
            def _():
                def keep(rows):
                    at = (i - (early - HELD)) * rows_per + rows.start
                    last_w[d, pl.ds(pl.multiple_of(at, 8), PIECE)] = wo[s, rows]

                pieces(keep)

            @pl.when(i >= early)
            def _():
                stores(i, late_w.at[i - early])[0].start()
                stores(i, late_twin.at[i - early])[3].start()

            for here, there in spots(i, d):

                @pl.when(here & (i < early))
                def _(there=there):
                    local, to_right, to_left, to_twin = stores(i, there)

                    @pl.when(z < CHIPS - 1)
                    def _():
                        to_right.start()

                    @pl.when(z > 0)
                    def _():
                        to_left.start()

                    to_twin.start()
                    if there.memory_space != pltpu.VMEM:
                        local.start()

    def forwards(i, o, to, there):
        a = lax.rem(i, S_AG)
        return remote(there, there, fwd_s.at[a, o], ag_r.at[a, o], to), remote(there, there, sib_s.at[a, o], sib_r.at[a, o], twin)

    def sent(i, o, to, on):
        ahead, across = forwards(i, o, to, spots(i, 0)[0][1])

        @pl.when(on)
        def _():
            ahead.wait_send()

        across.wait_send()

    def gathering(t, rightward):
        many, to, on = (z, right, z < CHIPS - 1) if rightward else (CHIPS - 1 - z, left, z > 0)

        def lane(k, _):
            o = z - 1 - k if rightward else z + 1 + k
            i = t - turn(o) - HOP2 * (k + 1)

            @pl.when((i >= 0) & (i < early))
            def _():
                @pl.when(i >= S_AG)
                def _():
                    sent(i - S_AG, o, to, on)

                forwards(i, o, to, spots(i, 0)[0][1])[0].wait_recv()
                for here, there in spots(i, o * 2 + c):

                    @pl.when(here)
                    def _(there=there):
                        ahead, across = forwards(i, o, to, there)

                        @pl.when(on)
                        def _():
                            ahead.start()

                        across.start()

            return 0

        lax.fori_loop(0, many, lane, 0)

    def crossing(t):
        def lane(o, _):
            i = t - turn(o) - HOP2 * jnp.abs(z - o) - 2

            @pl.when((i >= 0) & ((i < early) | (o == z) & (i < n)))
            def _():
                forwards(i, o, right, spots(i, 0)[0][1])[1].wait_recv()

            return 0

        lax.fori_loop(0, CHIPS, lane, 0)

    def step(t, _):
        passing(t, True)
        passing(t, False)
        adam(t)
        gathering(t, True)
        gathering(t, False)
        fetch(t)
        fetch_state(t)
        crossing(t)
        return 0

    lax.fori_loop(0, LAG + HOP * (CHIPS - 1) + max(n + 2, early + HOP2 * (CHIPS - 1) + 2) + 1, step, 0)

    def raw_left(k, _):
        raw(n - S_RAW + k)[1][0][1].wait_send()
        return 0

    lax.fori_loop(0, S_RAW, raw_left, 0)

    def pass_left(k, _):
        i = n - S_OUT + k
        s, e = lax.rem(i, S_OUT), lax.rem(i, S_IN)

        def to_right(o, _):
            remote(rout.at[s, o], rin.at[e, o], rs.at[s, o], rr.at[e, o], right).wait_send()
            return 0

        def to_left(o, _):
            remote(lout.at[s, o], lin.at[e, o], ls.at[s, o], lr.at[e, o], left).wait_send()
            return 0

        lax.fori_loop(z + 1, CHIPS, to_right, 0)
        lax.fori_loop(0, z, to_left, 0)
        return 0

    lax.fori_loop(0, S_OUT, pass_left, 0)

    def stores_left(k, _):
        stored(n - S_ADAM + k)
        return 0

    lax.fori_loop(0, S_ADAM, stores_left, 0)

    def gather_left(k, _):
        i = early - S_AG + k

        def of_left(o, _):
            sent(i, o, right, z < CHIPS - 1)
            return 0

        def of_right(o, _):
            sent(i, o, left, z > 0)
            return 0

        lax.fori_loop(0, z, of_left, 0)
        lax.fori_loop(z + 1, CHIPS, of_right, 0)
        return 0

    lax.fori_loop(0, S_AG, gather_left, 0)


def write_out(through, straight, held, in_sem, out_sem, sem):
    n, ahead = len(through), S_COPY - 3

    def slot(j):
        return held.at[j % S_COPY, pl.ds(0, through[j][0].shape[0])]

    def load(j):
        return pltpu.make_async_copy(through[j][0], slot(j), in_sem.at[j % S_COPY])

    def store(j):
        return pltpu.make_async_copy(slot(j), through[j][1], out_sem.at[j % S_COPY])

    rest = [pltpu.make_async_copy(*pair, sem.at[k]) for k, pair in enumerate(straight)]
    for j in range(ahead):
        load(j).start()
    for copy in rest:
        copy.start()
    for j in range(n):
        load(j).wait()
        store(j).start()
        if j + ahead < n:
            if j + ahead >= S_COPY:
                store(j + ahead - S_COPY).wait()
            load(j + ahead).start()
    for j in range(n - S_COPY, n):
        store(j).wait()
    for copy in rest:
        copy.wait()


def spans(source, target, rows):
    many = source.shape[0]
    return [(source.at[pl.ds(p, min(rows, many - p))], target.at[pl.ds(p, min(rows, many - p))]) for p in range(0, many, rows)]


def write_most(new_w, state, *refs):
    outs, (held, *sems) = refs[:9], refs[9:]
    _, layers, owners, block, _ = new_w.shape
    through = []
    for k in range(3):
        for layer in range(layers):
            there = pl.ds(0, block - (LATE + HELD) * TILES * 8 if (k, layer) == (2, layers - 1) else block)
            for owner in range(owners):
                through += spans(new_w.at[k, layer, owner, there], outs[k].at[layer, owner, there], held.shape[1])
    write_out(through, [(state.at[k // 3, k % 3], outs[3 + k]) for k in range(6)], held, *sems)


def write_held(so_far, last_w, out, sem):
    del so_far
    rows = TILES * 8
    copy = pltpu.make_async_copy(last_w, out.at[out.shape[0] - 1, :, pl.ds(out.shape[2] - (LATE + HELD) * rows, HELD * rows)], sem)
    copy.start()
    copy.wait()


def write_late(so_far, *refs):
    del so_far
    blocks, (out, sem) = refs[: 2 * CHIPS], refs[2 * CHIPS :]
    d = lax.axis_index("dp")
    z, c = lax.div(d, 2), lax.rem(d, 2)
    rows = blocks[0].shape[0]
    copies = []
    for k, block in enumerate(blocks):
        owner = lax.rem(z + CHIPS - k % CHIPS, CHIPS) * 2 + (c if k < CHIPS else 1 - c)
        copies.append(pltpu.make_async_copy(block, out.at[out.shape[0] - 1, owner, pl.ds(out.shape[2] - rows, rows)], sem.at[k]))
    for copy in copies:
        copy.start()
    for copy in copies:
        copy.wait()


def solution(mesh):
    bf16, f32 = jnp.bfloat16, jnp.float32

    def step(*arrays):
        terms, weights, m, v = (arrays[i : i + 3] for i in (0, 3, 6, 9))
        layers = weights[0].shape[0]
        block = weights[0].shape[1] * weights[0].shape[2] // (2 * CHIPS * 128)
        rows = TILES * 8
        args = [tiles(t[0]).reshape(layers, CHIPS, 2, block, 128) for t in terms]
        args += [tiles(w).reshape(layers, 2 * CHIPS, block, 128) for w in weights]
        args += [tiles(x) for x in (*m, *v)]
        dma = pltpu.SemaphoreType.DMA
        in_hbm, in_vmem = pl.BlockSpec(memory_space=pltpu.HBM), pl.BlockSpec(memory_space=pltpu.VMEM)
        new_w, last_w, late_w, late_twin, state = pl.pallas_call(
            functools.partial(kernel, block // rows, layers),
            out_shape=[
                jax.ShapeDtypeStruct((3, layers, 2 * CHIPS, block, 128), bf16),
                pltpu.VMEM((2 * CHIPS, HELD * rows, 128), bf16),
                jax.ShapeDtypeStruct((LATE, rows, 128), bf16),
                jax.ShapeDtypeStruct((LATE, rows, 128), bf16),
                pltpu.VMEM((2, 3, layers, block, 128), f32),
            ],
            in_specs=[in_hbm] * 12,
            out_specs=[in_hbm, in_vmem, in_hbm, in_hbm, in_vmem],
            scratch_shapes=[
                pltpu.VMEM((S_RAW, CHIPS, rows, 128), bf16),
                pltpu.VMEM((S_RAW, CHIPS, rows, 128), bf16),
                pltpu.VMEM((S_IN, CHIPS, rows, 128), bf16),
                pltpu.VMEM((S_IN, CHIPS, rows, 128), bf16),
                pltpu.VMEM((S_OUT, CHIPS, rows, 128), bf16),
                pltpu.VMEM((S_OUT, CHIPS, rows, 128), bf16),
                pltpu.VMEM((rows, 128), f32),
                pltpu.VMEM((S_ADAM, rows, 128), bf16),
                pltpu.VMEM((S_ADAM, rows, 128), bf16),
                dma((S_RAW,)),
                dma((S_RAW,)),
                dma((S_RAW,)),
                dma((S_OUT, CHIPS)),
                dma((S_IN, CHIPS)),
                dma((S_OUT, CHIPS)),
                dma((S_IN, CHIPS)),
                dma((S_ADAM, 3)),
                dma((S_ADAM,)),
                dma((S_ADAM, 3)),
                dma((S_AG, CHIPS)),
                dma((S_AG, CHIPS)),
                dma((S_AG, CHIPS)),
                dma((S_AG, CHIPS)),
            ],
            compiler_params=pltpu.CompilerParams(collective_id=0, has_side_effects=True, vmem_limit_bytes=ROOM),
        )(*(pltpu.with_memory_space_constraint(x, pltpu.HBM) for x in args))
        every = range(2 * CHIPS)
        every = range(2 * CHIPS)
        late = [late_w.reshape(LATE * rows, 128)]
        late += [lax.ppermute(late[0], "dp", [(d, (d + 2 * k) % (2 * CHIPS)) for d in every]) for k in range(1, CHIPS)]
        grant = pltpu.CompilerParams(vmem_limit_bytes=ROOM)
        most = pl.pallas_call(
            write_most,
            out_shape=[jax.ShapeDtypeStruct((layers, 2 * CHIPS, block, 128), bf16)] * 3 + [jax.ShapeDtypeStruct((layers, block, 128), f32)] * 6,
            in_specs=[in_hbm, in_vmem],
            out_specs=[in_hbm] * 9,
            scratch_shapes=[pltpu.VMEM((S_COPY, SPAN, 128), bf16), dma((S_COPY,)), dma((S_COPY,)), dma((6,))],
            compiler_params=grant,
            cost_estimate=pl.CostEstimate(flops=MOST_COST, bytes_accessed=150 * 10**6, transcendentals=0),
        )(new_w, state)
        twins = [late_twin.reshape(LATE * rows, 128)]
        twins += [lax.ppermute(x, "dp", [(d, d ^ 1) for d in every]) for x in late[1:]]
        last = pl.pallas_call(
            write_held,
            out_shape=jax.ShapeDtypeStruct(most[2].shape, bf16),
            in_specs=[in_hbm, in_vmem],
            out_specs=in_hbm,
            scratch_shapes=[dma],
            input_output_aliases={0: 0},
            compiler_params=grant,
            cost_estimate=pl.CostEstimate(flops=MOST_COST // 16, bytes_accessed=7 * 10**6, transcendentals=0),
        )(most[2], last_w)
        last = pl.pallas_call(
            write_late,
            out_shape=jax.ShapeDtypeStruct(last.shape, bf16),
            in_specs=[in_hbm] + [in_vmem] * (2 * CHIPS),
            out_specs=in_hbm,
            scratch_shapes=[dma((2 * CHIPS,))],
            input_output_aliases={0: 0},
            compiler_params=grant,
        )(last, *late, *twins)
        outs = [*(x.reshape(layers, -1, 128) for x in (most[0], most[1], last)), *most[3:]]
        outs = [untiles(o, *old.shape[1:]) for o, old in zip(outs, (*weights, *m, *v), strict=True)]
        return tuple(outs)

    all_of, cut = P(None, None, None), P(None, "dp", None)
    return jax.shard_map(
        step,
        mesh=mesh,
        in_specs=(P(("rep", "dp"), None, None, None),) * 3 + (all_of,) * 3 + (cut,) * 6,
        out_specs=(P("rep", None, None),) * 3 + (P("rep", "dp", None),) * 6,
        check_vma=False,
    )
```

```python
import functools

import jax
import jax.numpy as jnp
from jax import lax
from jax.experimental import pallas as pl
from jax.experimental.pallas import tpu as pltpu
from jax.sharding import PartitionSpec as P

MESH = pl.DeviceIdType.MESH
CHIPS = 4
TILES = 28
HOP = 1
HOP2 = 1
RUN = 2
LAG = 2
S_RAW, S_IN, S_OUT, S_ADAM, S_AG = 12, 8, 3, 3, 16
LATE = 9
ROOM = 11264 * 1024
SPAN, S_COPY = 2800, 12
MOST_COST = 10**11
PIECE = 32


def tiles(x):
    *lead, r, c = x.shape
    return x.reshape(*lead, r // 8, 8, c // 128, 128).swapaxes(-3, -2).reshape(*lead, r * c // 128, 128)


def untiles(x, r, c):
    lead = x.shape[:-2]
    return x.reshape(*lead, r // 8, c // 128, 8, 128).swapaxes(-3, -2).reshape(*lead, r, c)


def kernel(
    per_layer, layers, *refs
):
    g, w, m, v = (refs[i : i + 3] for i in (0, 3, 6, 9))
    new_w, last_w, late_w, late_twin, state = refs[12:17]
    new_m, new_v = state.at[0], state.at[1]
    own, sib, rin, lin, rout, lout, total, wi, wo = refs[17:26]
    own_sem, raw_s, raw_r, rs, rr, ls, lr, ld_sem, st_sem, own_s, fwd_s, ag_r, sib_s, sib_r = refs[26:]
    rows_per = TILES * 8
    n = len(g) * layers * per_layer
    early = n - LATE
    kept = n - layers * per_layer
    d = lax.axis_index("dp")
    z, c = lax.div(d, 2), lax.rem(d, 2)
    right, left, twin = {"dp": lax.rem(d + 2, 8)}, {"dp": lax.rem(d + 6, 8)}, {"dp": z * 2 + 1 - c}
    far = jnp.maximum(z, CHIPS - 1 - z)

    def turn(o):
        return LAG + HOP * jnp.maximum(o, CHIPS - 1 - o)

    def place(i):
        which, rest = lax.div(i, layers * per_layer), lax.rem(i, layers * per_layer)
        layer, k = lax.div(rest, per_layer), lax.rem(rest, per_layer)
        return which, layer, pl.ds(pl.multiple_of(k * rows_per, 8), rows_per)

    def spots(i, owner):
        which, layer, rows = place(i)
        at = pl.ds(pl.multiple_of((i - kept) * rows_per, 8), rows_per)
        return (i < kept, new_w.at[which, layer, owner, rows]), (i >= kept, last_w.at[owner, at])

    block_sized = new_w.at[0, 0, 0, pl.ds(0, rows_per)]

    def inside(i):
        return (i >= 0) & (i < n)

    def remote(src, dst, s, r, to):
        return pltpu.make_async_remote_copy(src, dst, s, r, device_id=to, device_id_type=MESH)

    def pieces(body):
        def one(p, _):
            body(pl.ds(pl.multiple_of(p * PIECE, 8), PIECE))
            return 0

        lax.fori_loop(0, rows_per // PIECE, one, 0)

    def f32(ref):
        return ref[...].astype(jnp.float32)

    barrier = pltpu.get_barrier_semaphore()

    @pl.when(z < CHIPS - 1)
    def _():
        pl.semaphore_signal(barrier, 1, device_id=right, device_id_type=MESH)

    @pl.when(z > 0)
    def _():
        pl.semaphore_signal(barrier, 1, device_id=left, device_id_type=MESH)

    pl.semaphore_signal(barrier, 1, device_id=twin, device_id_type=MESH)
    pl.semaphore_wait(barrier, 1 + (z > 0).astype(jnp.int32) + (z < CHIPS - 1).astype(jnp.int32))

    def raw(i):
        which, layer, rows = place(i)
        s = lax.rem(i, S_RAW)
        return which, [
            (
                pltpu.make_async_copy(one.at[layer, :, c, rows], own.at[s], own_sem.at[s]),
                remote(one.at[layer, :, 1 - c, rows], sib.at[s], raw_s.at[s], raw_r.at[s], twin),
            )
            for one in g
        ]

    def chunks(step, ahead, body):
        def upto(x):
            return jnp.clip(jnp.minimum(2 * x, x + ahead), 0, n)

        def one(i, _):
            body(i)
            return 0

        lax.fori_loop(upto(step), upto(step + 1), one, 0)

    def fetch(t):
        def one(i):
            which, copies = raw(i)

            @pl.when(i >= S_RAW)
            def _():
                copies[0][1].wait_send()

            for one, (mine, other) in enumerate(copies):

                @pl.when(which == one)
                def _():
                    other.start()
                    mine.start()

        chunks(t, RUN, one)

    def arrived(i):
        _, copies = raw(i)
        copies[0][0].wait()
        copies[0][1].wait_recv()

    def passes(i, o, rightward):
        s, e = lax.rem(i, S_OUT), lax.rem(i, S_IN)
        if rightward:
            return remote(rout.at[s, o], rin.at[e, o], rs.at[s, o], rr.at[e, o], right)
        return remote(lout.at[s, o], lin.at[e, o], ls.at[s, o], lr.at[e, o], left)

    def passing(t, rightward):
        if rightward:
            before, box, out = z, rin, rout
            many, has_in, first = CHIPS - 1 - z, z > 0, z <= 1
        else:
            before, box, out = CHIPS - 1 - z, lin, lout
            many, has_in, first = z, z < CHIPS - 1, z > 1
        now = t - LAG - HOP * before

        @pl.when(first)
        def _():
            chunks(now, RUN, arrived)

        def lane(k, _):
            o = CHIPS - 1 - k if rightward else k

            def one(i):
                raw_slot, in_slot, out_slot = lax.rem(i, S_RAW), lax.rem(i, S_IN), lax.rem(i, S_OUT)
                copy = passes(i, o, rightward)

                @pl.when(i >= S_OUT)
                def _():
                    copy.wait_send()

                @pl.when(has_in)
                def _():
                    copy.wait_recv()

                    def add(rows):
                        so_far = f32(own.at[raw_slot, o, rows]) + f32(sib.at[raw_slot, o, rows])
                        out[out_slot, o, rows] = (so_far + f32(box.at[in_slot, o, rows])).astype(jnp.bfloat16)

                    pieces(add)

                @pl.when(jnp.logical_not(has_in))
                def _():
                    def add(rows):
                        so_far = f32(own.at[raw_slot, o, rows]) + f32(sib.at[raw_slot, o, rows])
                        out[out_slot, o, rows] = so_far.astype(jnp.bfloat16)

                    pieces(add)

                copy.start()

            chunks(now, jnp.minimum(CHIPS - 2 - k, RUN), one)
            return 0

        lax.fori_loop(0, many, lane, 0)

    def loads(i):
        which, layer, rows = place(i)
        s = lax.rem(i, S_ADAM)
        return which, [
            (
                pltpu.make_async_copy(m[one].at[layer, rows], new_m.at[one, layer, rows], ld_sem.at[s, 0]),
                pltpu.make_async_copy(v[one].at[layer, rows], new_v.at[one, layer, rows], ld_sem.at[s, 1]),
                pltpu.make_async_copy(w[one].at[layer, d, rows], wi.at[s], ld_sem.at[s, 2]),
            )
            for one in range(3)
        ]

    def fetch_state(t):
        i = t - turn(z) + S_ADAM - 1

        @pl.when(inside(i))
        def _():
            which, copies = loads(i)
            for one, each in enumerate(copies):

                @pl.when(which == one)
                def _():
                    for copy in each:
                        copy.start()

    def stores(i, there):
        s, a = lax.rem(i, S_ADAM), lax.rem(i, S_AG)
        local = pltpu.make_async_copy(wo.at[s], there, st_sem.at[s])
        to_right = remote(wo.at[s], there, own_s.at[s, 0], ag_r.at[a, z], right)
        to_left = remote(wo.at[s], there, own_s.at[s, 1], ag_r.at[a, z], left)
        to_twin = remote(wo.at[s], there, own_s.at[s, 2], sib_r.at[a, z], twin)
        return local, to_right, to_left, to_twin

    def stored(i):
        local, to_right, to_left, to_twin = stores(i, block_sized)

        @pl.when((i < kept) | (i >= early))
        def _():
            local.wait()

        to_twin.wait_send()

        @pl.when((i < early) & (z < CHIPS - 1))
        def _():
            to_right.wait_send()

        @pl.when((i < early) & (z > 0))
        def _():
            to_left.wait_send()

    def adam(t):
        i = t - turn(z)

        @pl.when(inside(i))
        def _():
            raw_slot, in_slot, s = lax.rem(i, S_RAW), lax.rem(i, S_IN), lax.rem(i, S_ADAM)
            _, copies = loads(i)
            for copy in copies[0]:
                copy.wait()

            @pl.when(i >= S_ADAM)
            def _():
                stored(i - S_ADAM)

            def begin(rows):
                total[rows] = f32(own.at[raw_slot, z, rows]) + f32(sib.at[raw_slot, z, rows])

            pieces(begin)

            @pl.when(z > 0)
            def _():
                passes(i, z, True).wait_recv()

                def add(rows):
                    total[rows] += f32(rin.at[in_slot, z, rows])

                pieces(add)

            @pl.when(z < CHIPS - 1)
            def _():
                passes(i, z, False).wait_recv()

                def add(rows):
                    total[rows] += f32(lin.at[in_slot, z, rows])

                pieces(add)

            which, layer, base = place(i)

            def step(rows):
                to = pl.ds(pl.multiple_of(base.start + rows.start, 8), PIECE)
                grad = total[rows].astype(jnp.bfloat16).astype(jnp.float32)
                m1 = 0.9 * new_m[which, layer, to] + 0.1 * grad
                v1 = 0.95 * new_v[which, layer, to] + 0.05 * grad * grad
                w0 = f32(wi.at[s, rows])
                new_m[which, layer, to] = m1
                new_v[which, layer, to] = v1
                wo[s, rows] = (w0 - 0.02 * (m1 * lax.rsqrt(v1 + 1e-8) + 0.1 * w0)).astype(jnp.bfloat16)

            pieces(step)

            @pl.when((i >= kept) & (i < early))
            def _():
                def keep(rows):
                    at = (i - kept) * rows_per + rows.start
                    last_w[d, pl.ds(pl.multiple_of(at, 8), PIECE)] = wo[s, rows]

                pieces(keep)

            @pl.when(i >= early)
            def _():
                stores(i, late_w.at[i - early])[0].start()
                stores(i, late_twin.at[i - early])[3].start()

            for here, there in spots(i, d):

                @pl.when(here & (i < early))
                def _(there=there):
                    local, to_right, to_left, to_twin = stores(i, there)

                    @pl.when(z < CHIPS - 1)
                    def _():
                        to_right.start()

                    @pl.when(z > 0)
                    def _():
                        to_left.start()

                    to_twin.start()
                    if there.memory_space != pltpu.VMEM:
                        local.start()

    def forwards(i, o, to, there):
        a = lax.rem(i, S_AG)
        return remote(there, there, fwd_s.at[a, o], ag_r.at[a, o], to), remote(there, there, sib_s.at[a, o], sib_r.at[a, o], twin)

    def sent(i, o, to, on):
        ahead, across = forwards(i, o, to, block_sized)

        @pl.when(on)
        def _():
            ahead.wait_send()

        across.wait_send()

    def gathering(t, rightward):
        many, to, on = (z, right, z < CHIPS - 1) if rightward else (CHIPS - 1 - z, left, z > 0)

        def lane(k, _):
            o = z - 1 - k if rightward else z + 1 + k
            i = t - turn(o) - HOP2 * (k + 1)

            @pl.when((i >= 0) & (i < early))
            def _():
                @pl.when(i >= S_AG)
                def _():
                    sent(i - S_AG, o, to, on)

                forwards(i, o, to, block_sized)[0].wait_recv()
                for here, there in spots(i, o * 2 + c):

                    @pl.when(here)
                    def _(there=there):
                        ahead, across = forwards(i, o, to, there)

                        @pl.when(on)
                        def _():
                            ahead.start()

                        across.start()

            return 0

        lax.fori_loop(0, many, lane, 0)

    def crossing(t):
        def lane(o, _):
            i = t - turn(o) - HOP2 * jnp.abs(z - o) - 2

            @pl.when((i >= 0) & ((i < early) | (o == z) & (i < n)))
            def _():
                forwards(i, o, right, block_sized)[1].wait_recv()

            return 0

        lax.fori_loop(0, CHIPS, lane, 0)

    def step(t, _):
        passing(t, True)
        passing(t, False)
        adam(t)
        gathering(t, True)
        gathering(t, False)
        fetch(t)
        fetch_state(t)
        crossing(t)
        return 0

    lax.fori_loop(0, LAG + HOP * (CHIPS - 1) + max(n + 2, early + HOP2 * (CHIPS - 1) + 2) + 1, step, 0)

    def raw_left(k, _):
        raw(n - S_RAW + k)[1][0][1].wait_send()
        return 0

    lax.fori_loop(0, S_RAW, raw_left, 0)

    def pass_left(k, _):
        def to_right(o, _):
            passes(n - S_OUT + k, o, True).wait_send()
            return 0

        def to_left(o, _):
            passes(n - S_OUT + k, o, False).wait_send()
            return 0

        lax.fori_loop(z + 1, CHIPS, to_right, 0)
        lax.fori_loop(0, z, to_left, 0)
        return 0

    lax.fori_loop(0, S_OUT, pass_left, 0)

    def stores_left(k, _):
        stored(n - S_ADAM + k)
        return 0

    lax.fori_loop(0, S_ADAM, stores_left, 0)

    def gather_left(k, _):
        i = early - S_AG + k

        def of_left(o, _):
            sent(i, o, right, z < CHIPS - 1)
            return 0

        def of_right(o, _):
            sent(i, o, left, z > 0)
            return 0

        lax.fori_loop(0, z, of_left, 0)
        lax.fori_loop(z + 1, CHIPS, of_right, 0)
        return 0

    lax.fori_loop(0, S_AG, gather_left, 0)


def write_out(through, straight, held, in_sem, out_sem, sem):
    n, ahead = len(through), S_COPY - 3
    assert n >= S_COPY

    def slot(j):
        return held.at[j % S_COPY, pl.ds(0, through[j][0].shape[0])]

    def load(j):
        return pltpu.make_async_copy(through[j][0], slot(j), in_sem.at[j % S_COPY])

    def store(j):
        return pltpu.make_async_copy(slot(j), through[j][1], out_sem.at[j % S_COPY])

    rest = [pltpu.make_async_copy(*pair, sem.at[k]) for k, pair in enumerate(straight)]
    for j in range(ahead):
        load(j).start()
    for copy in rest:
        copy.start()
    for j in range(n):
        load(j).wait()
        store(j).start()
        if j + ahead < n:
            if j + ahead >= S_COPY:
                store(j + ahead - S_COPY).wait()
            load(j + ahead).start()
    for j in range(n - S_COPY, n):
        store(j).wait()
    for copy in rest:
        copy.wait()


def spans(source, target, rows):
    many = source.shape[0]
    return [(source.at[pl.ds(p, min(rows, many - p))], target.at[pl.ds(p, min(rows, many - p))]) for p in range(0, many, rows)]


def write_most(new_w, last_w, state, *refs):
    outs, (held, *sems) = refs[:9], refs[9:]
    layers, owners, block, _ = outs[2].shape
    through = []
    for k in range(2):
        for layer in range(layers):
            for owner in range(owners):
                through += spans(new_w.at[k, layer, owner], outs[k].at[layer, owner], held.shape[1])
    straight = [(last_w.at[:, pl.ds(layer * block, block)], outs[2].at[layer]) for layer in range(layers - 1)]
    straight += [(state.at[k // 3, k % 3], outs[3 + k]) for k in range(6)]
    write_out(through, straight, held, *sems)


def write_last(so_far, last_w, out, sem):
    del so_far
    layers, _, block, _ = out.shape
    done = (layers - 1) * block
    rest = last_w.shape[1] - done
    copy = pltpu.make_async_copy(last_w.at[:, pl.ds(done, rest)], out.at[layers - 1, :, pl.ds(0, rest)], sem)
    copy.start()
    copy.wait()


def write_late(so_far, *refs):
    del so_far
    blocks, (out, sem) = refs[: 2 * CHIPS], refs[2 * CHIPS :]
    d = lax.axis_index("dp")
    z, c = lax.div(d, 2), lax.rem(d, 2)
    rows = blocks[0].shape[0]
    copies = []
    for k, block in enumerate(blocks):
        owner = lax.rem(z + k, CHIPS) * 2 + (c if k < CHIPS else 1 - c)
        copies.append(pltpu.make_async_copy(block, out.at[out.shape[0] - 1, owner, pl.ds(out.shape[2] - rows, rows)], sem.at[k]))
    for copy in copies:
        copy.start()
    for copy in copies:
        copy.wait()


def solution(mesh):
    bf16, f32 = jnp.bfloat16, jnp.float32

    def step(*arrays):
        terms, weights, m, v = (arrays[i : i + 3] for i in (0, 3, 6, 9))
        layers = weights[0].shape[0]
        block = weights[0].shape[1] * weights[0].shape[2] // (2 * CHIPS * 128)
        rows = TILES * 8
        args = [tiles(t[0]).reshape(layers, CHIPS, 2, block, 128) for t in terms]
        args += [tiles(w).reshape(layers, 2 * CHIPS, block, 128) for w in weights]
        args += [tiles(x) for x in (*m, *v)]
        dma = pltpu.SemaphoreType.DMA
        in_hbm, in_vmem = pl.BlockSpec(memory_space=pltpu.HBM), pl.BlockSpec(memory_space=pltpu.VMEM)
        new_w, last_w, late_w, late_twin, state = pl.pallas_call(
            functools.partial(kernel, block // rows, layers),
            out_shape=[
                jax.ShapeDtypeStruct((2, layers, 2 * CHIPS, block, 128), bf16),
                pltpu.VMEM((2 * CHIPS, layers * block - LATE * rows, 128), bf16),
                jax.ShapeDtypeStruct((LATE, rows, 128), bf16),
                jax.ShapeDtypeStruct((LATE, rows, 128), bf16),
                pltpu.VMEM((2, 3, layers, block, 128), f32),
            ],
            in_specs=[in_hbm] * 12,
            out_specs=[in_hbm, in_vmem, in_hbm, in_hbm, in_vmem],
            scratch_shapes=[
                pltpu.VMEM((S_RAW, CHIPS, rows, 128), bf16),
                pltpu.VMEM((S_RAW, CHIPS, rows, 128), bf16),
                pltpu.VMEM((S_IN, CHIPS, rows, 128), bf16),
                pltpu.VMEM((S_IN, CHIPS, rows, 128), bf16),
                pltpu.VMEM((S_OUT, CHIPS, rows, 128), bf16),
                pltpu.VMEM((S_OUT, CHIPS, rows, 128), bf16),
                pltpu.VMEM((rows, 128), f32),
                pltpu.VMEM((S_ADAM, rows, 128), bf16),
                pltpu.VMEM((S_ADAM, rows, 128), bf16),
                dma((S_RAW,)),
                dma((S_RAW,)),
                dma((S_RAW,)),
                dma((S_OUT, CHIPS)),
                dma((S_IN, CHIPS)),
                dma((S_OUT, CHIPS)),
                dma((S_IN, CHIPS)),
                dma((S_ADAM, 3)),
                dma((S_ADAM,)),
                dma((S_ADAM, 3)),
                dma((S_AG, CHIPS)),
                dma((S_AG, CHIPS)),
                dma((S_AG, CHIPS)),
                dma((S_AG, CHIPS)),
            ],
            compiler_params=pltpu.CompilerParams(collective_id=0, has_side_effects=True, vmem_limit_bytes=ROOM),
        )(*(pltpu.with_memory_space_constraint(x, pltpu.HBM) for x in args))
        last_w, state = (pltpu.with_memory_space_constraint(x, pltpu.VMEM) for x in (last_w, state))
        every = range(2 * CHIPS)
        every = range(2 * CHIPS)
        late = [late_w.reshape(LATE * rows, 128)]
        late += [lax.ppermute(late[0], "dp", [((d + 2 * k) % (2 * CHIPS), d) for d in every]) for k in range(1, CHIPS)]
        grant = pltpu.CompilerParams(vmem_limit_bytes=ROOM)
        most = pl.pallas_call(
            write_most,
            out_shape=[jax.ShapeDtypeStruct((layers, 2 * CHIPS, block, 128), bf16)] * 3 + [jax.ShapeDtypeStruct((layers, block, 128), f32)] * 6,
            in_specs=[in_hbm, in_vmem, in_vmem],
            out_specs=[in_hbm] * 9,
            scratch_shapes=[pltpu.VMEM((S_COPY, SPAN, 128), bf16), dma((S_COPY,)), dma((S_COPY,)), dma((5 + layers,))],
            compiler_params=grant,
            cost_estimate=pl.CostEstimate(flops=MOST_COST, bytes_accessed=150 * 10**6, transcendentals=0),
        )(new_w, last_w, state)
        twins = [late_twin.reshape(LATE * rows, 128)]
        twins += [lax.ppermute(x, "dp", [(d, d ^ 1) for d in every]) for x in late[1:]]
        last = pl.pallas_call(
            write_last,
            out_shape=jax.ShapeDtypeStruct(most[2].shape, bf16),
            in_specs=[in_hbm, in_vmem],
            out_specs=in_hbm,
            scratch_shapes=[dma],
            input_output_aliases={0: 0},
            compiler_params=grant,
            cost_estimate=pl.CostEstimate(flops=MOST_COST // 16, bytes_accessed=7 * 10**6, transcendentals=0),
        )(most[2], last_w)
        last = pl.pallas_call(
            write_late,
            out_shape=jax.ShapeDtypeStruct(last.shape, bf16),
            in_specs=[in_hbm] + [in_vmem] * (2 * CHIPS),
            out_specs=in_hbm,
            scratch_shapes=[dma((2 * CHIPS,))],
            input_output_aliases={0: 0},
            compiler_params=grant,
        )(last, *late, *twins)
        outs = [*(x.reshape(layers, -1, 128) for x in (most[0], most[1], last)), *most[3:]]
        outs = [untiles(o, *old.shape[1:]) for o, old in zip(outs, (*weights, *m, *v), strict=True)]
        return tuple(outs)

    all_of, cut = P(None, None, None), P(None, "dp", None)
    return jax.shard_map(
        step,
        mesh=mesh,
        in_specs=(P(("rep", "dp"), None, None, None),) * 3 + (all_of,) * 3 + (cut,) * 6,
        out_specs=(P("rep", None, None),) * 3 + (P("rep", "dp", None),) * 6,
        check_vma=False,
    )
```

```python
import functools

import jax
import jax.numpy as jnp
from jax import lax
from jax.experimental import pallas as pl
from jax.experimental.pallas import tpu as pltpu
from jax.sharding import PartitionSpec as P

MESH = pl.DeviceIdType.MESH
CHIPS = 4
TILES = 28
HOP = 1
HOP2 = 1
RUN = 2
LAG = 2
S_RAW, S_IN, S_OUT, S_ADAM, S_AG = 12, 8, 3, 3, 16
SENT = 5
LATE = 9
ROOM = 11264 * 1024
SPAN, S_COPY = 2800, 12
MOST_COST = 10**11
AWAY = 0, 1, 3, 2
PIECE = 32


def tiles(x):
    *lead, r, c = x.shape
    return x.reshape(*lead, r // 8, 8, c // 128, 128).swapaxes(-3, -2).reshape(*lead, r * c // 128, 128)


def untiles(x, r, c):
    lead = x.shape[:-2]
    return x.reshape(*lead, r // 8, c // 128, 8, 128).swapaxes(-3, -2).reshape(*lead, r, c)


def kernel(
    per_layer, layers, *refs
):
    g, w, m, v = (refs[i : i + 3] for i in (0, 3, 6, 9))
    new_w, last_w, late_w, late_twin, state = refs[12:17]
    new_m, new_v = state.at[0], state.at[1]
    own, sib, rin, lin, rout, lout, total, wi, wo = refs[17:26]
    own_sem, raw_s, raw_r, rs, rr, ls, lr, ld_sem, st_sem, own_s, fwd_s, ag_r, sib_s, sib_r = refs[26:]
    rows_per = TILES * 8
    n = len(g) * layers * per_layer
    early = n - LATE
    kept = n - layers * per_layer
    d = lax.axis_index("dp")
    z, c = lax.div(d, 2), lax.rem(d, 2)
    right, left, twin = {"dp": lax.rem(d + 2, 8)}, {"dp": lax.rem(d + 6, 8)}, {"dp": z * 2 + 1 - c}
    far = jnp.maximum(z, CHIPS - 1 - z)

    def turn(o):
        return LAG + HOP * jnp.maximum(o, CHIPS - 1 - o)

    def place(i):
        which, rest = lax.div(i, layers * per_layer), lax.rem(i, layers * per_layer)
        layer, k = lax.div(rest, per_layer), lax.rem(rest, per_layer)
        return which, layer, pl.ds(pl.multiple_of(k * rows_per, 8), rows_per)

    def spots(i, owner):
        which, layer, rows = place(i)
        at = pl.ds(pl.multiple_of((i - kept) * rows_per, 8), rows_per)
        return (i < kept, new_w.at[which, layer, owner, rows]), (i >= kept, last_w.at[owner, at])

    block_sized = new_w.at[0, 0, 0, pl.ds(0, rows_per)]

    def inside(i):
        return (i >= 0) & (i < n)

    def remote(src, dst, s, r, to):
        return pltpu.make_async_remote_copy(src, dst, s, r, device_id=to, device_id_type=MESH)

    def pieces(body):
        def one(p, _):
            body(pl.ds(pl.multiple_of(p * PIECE, 8), PIECE))
            return 0

        lax.fori_loop(0, rows_per // PIECE, one, 0)

    def f32(ref):
        return ref[...].astype(jnp.float32)

    barrier = pltpu.get_barrier_semaphore()

    @pl.when(z < CHIPS - 1)
    def _():
        pl.semaphore_signal(barrier, 1, device_id=right, device_id_type=MESH)

    @pl.when(z > 0)
    def _():
        pl.semaphore_signal(barrier, 1, device_id=left, device_id_type=MESH)

    pl.semaphore_signal(barrier, 1, device_id=twin, device_id_type=MESH)
    pl.semaphore_wait(barrier, 1 + (z > 0).astype(jnp.int32) + (z < CHIPS - 1).astype(jnp.int32))

    def raw(i):
        which, layer, rows = place(i)
        s = lax.rem(i, S_RAW)
        return which, [
            (
                pltpu.make_async_copy(one.at[layer, :, c, rows], own.at[s], own_sem.at[s]),
                remote(one.at[layer, :, 1 - c, rows], sib.at[s], raw_s.at[s], raw_r.at[s], twin),
            )
            for one in g
        ]

    def chunks(step, ahead, body):
        def upto(x):
            return jnp.clip(jnp.minimum(2 * x, x + ahead), 0, n)

        def one(i, _):
            body(i)
            return 0

        lax.fori_loop(upto(step), upto(step + 1), one, 0)

    def fetch(t):
        def one(i):
            which, copies = raw(i)
            for one, (mine, other) in enumerate(copies):

                @pl.when(which == one)
                def _():
                    other.start()
                    mine.start()

        chunks(t, RUN, one)

    def arrived(i):
        _, copies = raw(i)
        copies[0][0].wait()
        copies[0][1].wait_recv()

    def passes(i, o, rightward):
        s, e = lax.rem(i, S_OUT), lax.rem(i, S_IN)
        if rightward:
            return remote(rout.at[s, o], rin.at[e, o], rs.at[s, o], rr.at[e, o], right)
        return remote(lout.at[s, o], lin.at[e, o], ls.at[s, o], lr.at[e, o], left)

    def passing(t, rightward):
        if rightward:
            before, box, out = z, rin, rout
            many, has_in, first = CHIPS - 1 - z, z > 0, z <= 1
        else:
            before, box, out = CHIPS - 1 - z, lin, lout
            many, has_in, first = z, z < CHIPS - 1, z > 1
        now = t - LAG - HOP * before

        @pl.when(first)
        def _():
            chunks(now, RUN, arrived)

        def lane(k, _):
            o = CHIPS - 1 - k if rightward else k

            def one(i):
                raw_slot, in_slot, out_slot = lax.rem(i, S_RAW), lax.rem(i, S_IN), lax.rem(i, S_OUT)
                copy = passes(i, o, rightward)

                @pl.when(i >= S_OUT)
                def _():
                    copy.wait_send()

                @pl.when(has_in)
                def _():
                    copy.wait_recv()

                    def add(rows):
                        so_far = f32(own.at[raw_slot, o, rows]) + f32(sib.at[raw_slot, o, rows])
                        out[out_slot, o, rows] = (so_far + f32(box.at[in_slot, o, rows])).astype(jnp.bfloat16)

                    pieces(add)

                @pl.when(jnp.logical_not(has_in))
                def _():
                    def add(rows):
                        so_far = f32(own.at[raw_slot, o, rows]) + f32(sib.at[raw_slot, o, rows])
                        out[out_slot, o, rows] = so_far.astype(jnp.bfloat16)

                    pieces(add)

                copy.start()

            chunks(now, jnp.minimum(CHIPS - 2 - k, RUN), one)
            return 0

        lax.fori_loop(0, many, lane, 0)

    def loads(i):
        which, layer, rows = place(i)
        s = lax.rem(i, S_ADAM)
        return which, [
            (
                pltpu.make_async_copy(m[one].at[layer, rows], new_m.at[one, layer, rows], ld_sem.at[s, 0]),
                pltpu.make_async_copy(v[one].at[layer, rows], new_v.at[one, layer, rows], ld_sem.at[s, 1]),
                pltpu.make_async_copy(w[one].at[layer, d, rows], wi.at[s], ld_sem.at[s, 2]),
            )
            for one in range(3)
        ]

    def fetch_state(t):
        i = t - turn(z) + S_ADAM - 1

        @pl.when(inside(i))
        def _():
            which, copies = loads(i)
            for one, each in enumerate(copies):

                @pl.when(which == one)
                def _():
                    for copy in each:
                        copy.start()

    def stores(i, there):
        s, a = lax.rem(i, S_ADAM), lax.rem(i, S_AG)
        local = pltpu.make_async_copy(wo.at[s], there, st_sem.at[s])
        to_right = remote(wo.at[s], there, own_s.at[s, 0], ag_r.at[a, z], right)
        to_left = remote(wo.at[s], there, own_s.at[s, 1], ag_r.at[a, z], left)
        to_twin = remote(wo.at[s], there, own_s.at[s, 2], sib_r.at[a, z], twin)
        return local, to_right, to_left, to_twin

    def stored(i):
        local, to_right, to_left, to_twin = stores(i, block_sized)

        @pl.when((i < kept) | (i >= early))
        def _():
            local.wait()

        to_twin.wait_send()

        @pl.when((i < early) & (z < CHIPS - 1))
        def _():
            to_right.wait_send()

        @pl.when((i < early) & (z > 0))
        def _():
            to_left.wait_send()

    def adam(t):
        i = t - turn(z)

        @pl.when(inside(i))
        def _():
            raw_slot, in_slot, s = lax.rem(i, S_RAW), lax.rem(i, S_IN), lax.rem(i, S_ADAM)
            _, copies = loads(i)
            for copy in copies[0]:
                copy.wait()

            raw(i)[1][0][1].wait_send()

            @pl.when(i >= S_ADAM)
            def _():
                stored(i - S_ADAM)

            @pl.when(z > 0)
            def _():
                passes(i, z, True).wait_recv()

            @pl.when(z < CHIPS - 1)
            def _():
                passes(i, z, False).wait_recv()

            def add(boxes):
                def one(rows):
                    so_far = f32(own.at[raw_slot, z, rows]) + f32(sib.at[raw_slot, z, rows])
                    for box in boxes:
                        so_far += f32(box.at[in_slot, z, rows])
                    total[rows] = so_far

                pieces(one)

            for here, boxes in ((z == 0, [lin]), (z == CHIPS - 1, [rin]), ((z > 0) & (z < CHIPS - 1), [rin, lin])):

                @pl.when(here)
                def _(boxes=boxes):
                    add(boxes)

            which, layer, base = place(i)

            def step(rows):
                to = pl.ds(pl.multiple_of(base.start + rows.start, 8), PIECE)
                grad = total[rows].astype(jnp.bfloat16).astype(jnp.float32)
                m1 = 0.9 * new_m[which, layer, to] + 0.1 * grad
                v1 = 0.95 * new_v[which, layer, to] + 0.05 * grad * grad
                w0 = f32(wi.at[s, rows])
                new_m[which, layer, to] = m1
                new_v[which, layer, to] = v1
                wo[s, rows] = (w0 - 0.02 * (m1 * lax.rsqrt(v1 + 1e-8) + 0.1 * w0)).astype(jnp.bfloat16)

            pieces(step)

            @pl.when((i >= kept) & (i < early))
            def _():
                def keep(rows):
                    at = (i - kept) * rows_per + rows.start
                    last_w[d, pl.ds(pl.multiple_of(at, 8), PIECE)] = wo[s, rows]

                pieces(keep)

            @pl.when(i >= early)
            def _():
                stores(i, late_w.at[i - early])[0].start()
                stores(i, late_twin.at[i - early])[3].start()

            for here, there in spots(i, d):

                @pl.when(here & (i < early))
                def _(there=there):
                    local, to_right, to_left, to_twin = stores(i, there)

                    @pl.when(z < CHIPS - 1)
                    def _():
                        to_right.start()

                    @pl.when(z > 0)
                    def _():
                        to_left.start()

                    to_twin.start()
                    if there.memory_space != pltpu.VMEM:
                        local.start()

    def forwards(i, o, to, there):
        a = lax.rem(i, S_AG)
        return remote(there, there, fwd_s.at[a, o], ag_r.at[a, o], to), remote(there, there, sib_s.at[a, o], sib_r.at[a, o], twin)

    def sent(i, o, to, on):
        ahead, across = forwards(i, o, to, block_sized)

        @pl.when(on)
        def _():
            ahead.wait_send()

        across.wait_send()

    def gathering(t, rightward):
        many, to, on = (z, right, z < CHIPS - 1) if rightward else (CHIPS - 1 - z, left, z > 0)

        def lane(k, _):
            o = z - 1 - k if rightward else z + 1 + k
            i = t - turn(o) - HOP2 * (k + 1)

            @pl.when((i >= SENT) & (i < early + SENT))
            def _():
                sent(i - SENT, o, to, on)

            @pl.when((i >= 0) & (i < early))
            def _():
                forwards(i, o, to, block_sized)[0].wait_recv()
                for here, there in spots(i, o * 2 + c):

                    @pl.when(here)
                    def _(there=there):
                        ahead, across = forwards(i, o, to, there)

                        @pl.when(on)
                        def _():
                            ahead.start()

                        across.start()

            return 0

        lax.fori_loop(0, many, lane, 0)

    def crossing(t):
        def lane(o, _):
            i = t - turn(o) - HOP2 * jnp.abs(z - o) - 2

            @pl.when((i >= 0) & (i < early))
            def _():
                forwards(i, o, right, block_sized)[1].wait_recv()

            return 0

        lax.fori_loop(0, CHIPS, lane, 0)

    def step(t, _):
        passing(t, True)
        passing(t, False)
        adam(t)
        gathering(t, True)
        gathering(t, False)
        fetch(t)
        fetch_state(t)
        crossing(t)
        return 0

    lax.fori_loop(0, LAG + HOP * (CHIPS - 1) + max(n, early + HOP2 * (CHIPS - 1) + max(2, SENT)), step, 0)

    def pass_left(k, _):
        def to_right(o, _):
            passes(n - S_OUT + k, o, True).wait_send()
            return 0

        def to_left(o, _):
            passes(n - S_OUT + k, o, False).wait_send()
            return 0

        lax.fori_loop(z + 1, CHIPS, to_right, 0)
        lax.fori_loop(0, z, to_left, 0)
        return 0

    lax.fori_loop(0, S_OUT, pass_left, 0)

    def stores_left(k, _):
        stored(n - S_ADAM + k)
        return 0

    lax.fori_loop(0, S_ADAM, stores_left, 0)

    def late_left(k, _):
        forwards(early + k, z, right, block_sized)[1].wait_recv()
        return 0

    lax.fori_loop(0, LATE, late_left, 0)


def write_out(through, straight, held, in_sem, out_sem, sem):
    n, ahead = len(through), S_COPY - 3
    assert n >= S_COPY

    def slot(j):
        return held.at[j % S_COPY, pl.ds(0, through[j][0].shape[0])]

    def load(j):
        return pltpu.make_async_copy(through[j][0], slot(j), in_sem.at[j % S_COPY])

    def store(j):
        return pltpu.make_async_copy(slot(j), through[j][1], out_sem.at[j % S_COPY])

    rest = [pltpu.make_async_copy(*pair, sem.at[k]) for k, pair in enumerate(straight)]
    for j in range(ahead):
        load(j).start()
    for j in range(n):
        load(j).wait()
        store(j).start()
        if j + ahead < n:
            if j + ahead >= S_COPY:
                store(j + ahead - S_COPY).wait()
            load(j + ahead).start()
    for copy in rest:
        copy.start()
    for j in range(n - S_COPY, n):
        store(j).wait()
    for copy in rest:
        copy.wait()


def spans(source, target, rows):
    many = source.shape[0]
    return [(source.at[pl.ds(p, min(rows, many - p))], target.at[pl.ds(p, min(rows, many - p))]) for p in range(0, many, rows)]


def write_most(new_w, last_w, state, *refs):
    outs, (held, *sems) = refs[:9], refs[9:]
    layers, owners, block, _ = outs[2].shape
    through = []
    for k in range(2):
        for layer in range(layers):
            for owner in range(owners):
                through += spans(new_w.at[k, layer, owner], outs[k].at[layer, owner], held.shape[1])
    straight = [(last_w.at[:, pl.ds(layer * block, block)], outs[2].at[layer]) for layer in range(layers - 1)]
    straight += [(state.at[k // 3, k % 3], outs[3 + k]) for k in range(6)]
    write_out(through, straight, held, *sems)


def write_last(so_far, last_w, out, sem):
    del so_far
    layers, _, block, _ = out.shape
    done = (layers - 1) * block
    rest = last_w.shape[1] - done
    copy = pltpu.make_async_copy(last_w.at[:, pl.ds(done, rest)], out.at[layers - 1, :, pl.ds(0, rest)], sem)
    copy.start()
    copy.wait()


def write_late(so_far, *refs):
    del so_far
    blocks, (out, sem) = refs[: 2 * CHIPS], refs[2 * CHIPS :]
    d = lax.axis_index("dp")
    z, c = lax.div(d, 2), lax.rem(d, 2)
    rows = blocks[0].shape[0]
    copies = []
    for k, block in enumerate(blocks):
        owner = lax.rem(z + AWAY[k % CHIPS], CHIPS) * 2 + (c if k < CHIPS else 1 - c)
        copies.append(pltpu.make_async_copy(block, out.at[out.shape[0] - 1, owner, pl.ds(out.shape[2] - rows, rows)], sem.at[k]))
    for copy in copies:
        copy.start()
    for copy in copies:
        copy.wait()


def solution(mesh):
    bf16, f32 = jnp.bfloat16, jnp.float32

    def step(*arrays):
        terms, weights, m, v = (arrays[i : i + 3] for i in (0, 3, 6, 9))
        layers = weights[0].shape[0]
        block = weights[0].shape[1] * weights[0].shape[2] // (2 * CHIPS * 128)
        rows = TILES * 8
        args = [tiles(t[0]).reshape(layers, CHIPS, 2, block, 128) for t in terms]
        args += [tiles(w).reshape(layers, 2 * CHIPS, block, 128) for w in weights]
        args += [tiles(x) for x in (*m, *v)]
        dma = pltpu.SemaphoreType.DMA
        in_hbm, in_vmem = pl.BlockSpec(memory_space=pltpu.HBM), pl.BlockSpec(memory_space=pltpu.VMEM)
        new_w, last_w, late_w, late_twin, state = pl.pallas_call(
            functools.partial(kernel, block // rows, layers),
            out_shape=[
                jax.ShapeDtypeStruct((2, layers, 2 * CHIPS, block, 128), bf16),
                pltpu.VMEM((2 * CHIPS, layers * block - LATE * rows, 128), bf16),
                jax.ShapeDtypeStruct((LATE, rows, 128), bf16),
                jax.ShapeDtypeStruct((LATE, rows, 128), bf16),
                pltpu.VMEM((2, 3, layers, block, 128), f32),
            ],
            in_specs=[in_hbm] * 12,
            out_specs=[in_hbm, in_vmem, in_hbm, in_hbm, in_vmem],
            scratch_shapes=[
                pltpu.VMEM((S_RAW, CHIPS, rows, 128), bf16),
                pltpu.VMEM((S_RAW, CHIPS, rows, 128), bf16),
                pltpu.VMEM((S_IN, CHIPS, rows, 128), bf16),
                pltpu.VMEM((S_IN, CHIPS, rows, 128), bf16),
                pltpu.VMEM((S_OUT, CHIPS, rows, 128), bf16),
                pltpu.VMEM((S_OUT, CHIPS, rows, 128), bf16),
                pltpu.VMEM((rows, 128), f32),
                pltpu.VMEM((S_ADAM, rows, 128), bf16),
                pltpu.VMEM((S_ADAM, rows, 128), bf16),
                dma((S_RAW,)),
                dma((S_RAW,)),
                dma((S_RAW,)),
                dma((S_OUT, CHIPS)),
                dma((S_IN, CHIPS)),
                dma((S_OUT, CHIPS)),
                dma((S_IN, CHIPS)),
                dma((S_ADAM, 3)),
                dma((S_ADAM,)),
                dma((S_ADAM, 3)),
                dma((S_AG, CHIPS)),
                dma((S_AG, CHIPS)),
                dma((S_AG, CHIPS)),
                dma((S_AG, CHIPS)),
            ],
            compiler_params=pltpu.CompilerParams(collective_id=0, has_side_effects=True, vmem_limit_bytes=ROOM),
        )(*(pltpu.with_memory_space_constraint(x, pltpu.HBM) for x in args))
        last_w, state = (pltpu.with_memory_space_constraint(x, pltpu.VMEM) for x in (last_w, state))
        every = range(2 * CHIPS)
        every = range(2 * CHIPS)
        late = [late_w.reshape(LATE * rows, 128)]
        late += [lax.ppermute(late[0], "dp", [((d + 2 * k) % (2 * CHIPS), d) for d in every]) for k in AWAY[1:]]
        grant = pltpu.CompilerParams(vmem_limit_bytes=ROOM)
        most = pl.pallas_call(
            write_most,
            out_shape=[jax.ShapeDtypeStruct((layers, 2 * CHIPS, block, 128), bf16)] * 3 + [jax.ShapeDtypeStruct((layers, block, 128), f32)] * 6,
            in_specs=[in_hbm, in_vmem, in_vmem],
            out_specs=[in_hbm] * 9,
            scratch_shapes=[pltpu.VMEM((S_COPY, SPAN, 128), bf16), dma((S_COPY,)), dma((S_COPY,)), dma((5 + layers,))],
            compiler_params=grant,
            cost_estimate=pl.CostEstimate(flops=MOST_COST, bytes_accessed=150 * 10**6, transcendentals=0),
        )(new_w, last_w, state)
        twins = [late_twin.reshape(LATE * rows, 128)]
        twins += [lax.ppermute(x, "dp", [(d, d ^ 1) for d in every]) for x in late[1:]]
        last = pl.pallas_call(
            write_last,
            out_shape=jax.ShapeDtypeStruct(most[2].shape, bf16),
            in_specs=[in_hbm, in_vmem],
            out_specs=in_hbm,
            scratch_shapes=[dma],
            input_output_aliases={0: 0},
            compiler_params=grant,
            cost_estimate=pl.CostEstimate(flops=MOST_COST // 16, bytes_accessed=7 * 10**6, transcendentals=0),
        )(most[2], last_w)
        last = pl.pallas_call(
            write_late,
            out_shape=jax.ShapeDtypeStruct(last.shape, bf16),
            in_specs=[in_hbm] + [in_vmem] * (2 * CHIPS),
            out_specs=in_hbm,
            scratch_shapes=[dma((2 * CHIPS,))],
            input_output_aliases={0: 0},
            compiler_params=grant,
        )(last, *late, *twins)
        outs = [*(x.reshape(layers, -1, 128) for x in (most[0], most[1], last)), *most[3:]]
        outs = [untiles(o, *old.shape[1:]) for o, old in zip(outs, (*weights, *m, *v), strict=True)]
        return tuple(outs)

    all_of, cut = P(None, None, None), P(None, "dp", None)
    return jax.shard_map(
        step,
        mesh=mesh,
        in_specs=(P(("rep", "dp"), None, None, None),) * 3 + (all_of,) * 3 + (cut,) * 6,
        out_specs=(P("rep", None, None),) * 3 + (P("rep", "dp", None),) * 6,
        check_vma=False,
    )
```

```python
import functools

import jax
import jax.numpy as jnp
from jax import lax
from jax.experimental import pallas as pl
from jax.experimental.pallas import tpu as pltpu
from jax.sharding import PartitionSpec as P

MESH = pl.DeviceIdType.MESH
CHIPS = 4
TILES = 35
HOP = 1
HOP2 = 1
RUN = 2
LAG = 1
S_RAW, S_IN, S_OUT, S_ADAM, S_AG = 8, 7, 2, 3, 16
SENT = 5
MORE = 4
LATE = 7
ROOM = 8960 * 1024
SPAN, S_COPY = 1400, 24
MOST_COST = 10**11
AWAY = 0, 1, 3, 2
PIECE = 40


def tiles(x):
    *lead, r, c = x.shape
    return x.reshape(*lead, r // 8, 8, c // 128, 128).swapaxes(-3, -2).reshape(*lead, r * c // 128, 128)


def untiles(x, r, c):
    lead = x.shape[:-2]
    return x.reshape(*lead, r // 8, c // 128, 8, 128).swapaxes(-3, -2).reshape(*lead, r, c)


def kernel(
    per_layer, layers, *refs
):
    g, w, m, v = (refs[i : i + 3] for i in (0, 3, 6, 9))
    new_w, last_w, late_w, late_twin, state = refs[12:17]
    new_m, new_v = state.at[0], state.at[1]
    own, sib, rin, lin, rout, lout, total, wi, wo = refs[17:26]
    own_sem, raw_s, raw_r, rs, rr, ls, lr, ld_sem, st_sem, own_s, fwd_s, ag_r, sib_s, sib_r = refs[26:]
    rows_per = TILES * 8
    n = len(g) * layers * per_layer
    early = n - LATE
    kept = n - layers * per_layer - MORE
    d = lax.axis_index("dp")
    z, c = lax.div(d, 2), lax.rem(d, 2)
    right, left, twin = {"dp": lax.rem(d + 2, 8)}, {"dp": lax.rem(d + 6, 8)}, {"dp": z * 2 + 1 - c}
    far = jnp.maximum(z, CHIPS - 1 - z)

    def turn(o):
        return LAG + HOP * jnp.maximum(o, CHIPS - 1 - o)

    def place(i):
        which, rest = lax.div(i, layers * per_layer), lax.rem(i, layers * per_layer)
        layer, k = lax.div(rest, per_layer), lax.rem(rest, per_layer)
        return which, layer, pl.ds(pl.multiple_of(k * rows_per, 8), rows_per)

    def spots(i, owner):
        which, layer, rows = place(i)
        at = pl.ds(pl.multiple_of((i - kept) * rows_per, 8), rows_per)
        return (i < kept, new_w.at[which, layer, owner, rows]), (i >= kept, last_w.at[owner, at])

    block_sized = new_w.at[0, 0, 0, pl.ds(0, rows_per)]

    def inside(i):
        return (i >= 0) & (i < n)

    def remote(src, dst, s, r, to):
        return pltpu.make_async_remote_copy(src, dst, s, r, device_id=to, device_id_type=MESH)

    def pieces(body):
        def one(p, _):
            body(pl.ds(pl.multiple_of(p * PIECE, 8), PIECE))
            return 0

        lax.fori_loop(0, rows_per // PIECE, one, 0)

    def f32(ref):
        return ref[...].astype(jnp.float32)

    barrier = pltpu.get_barrier_semaphore()

    @pl.when(z < CHIPS - 1)
    def _():
        pl.semaphore_signal(barrier, 1, device_id=right, device_id_type=MESH)

    @pl.when(z > 0)
    def _():
        pl.semaphore_signal(barrier, 1, device_id=left, device_id_type=MESH)

    pl.semaphore_signal(barrier, 1, device_id=twin, device_id_type=MESH)
    pl.semaphore_wait(barrier, 1 + (z > 0).astype(jnp.int32) + (z < CHIPS - 1).astype(jnp.int32))

    def raw(i):
        which, layer, rows = place(i)
        s = lax.rem(i, S_RAW)
        return which, [
            (
                pltpu.make_async_copy(one.at[layer, :, c, rows], own.at[s], own_sem.at[s]),
                remote(one.at[layer, :, 1 - c, rows], sib.at[s], raw_s.at[s], raw_r.at[s], twin),
            )
            for one in g
        ]

    def chunks(step, ahead, body):
        def upto(x):
            return jnp.clip(jnp.minimum(2 * x, x + ahead), 0, n)

        def one(i, _):
            body(i)
            return 0

        lax.fori_loop(upto(step), upto(step + 1), one, 0)

    def fetch(t):
        def one(i):
            which, copies = raw(i)
            for one, (mine, other) in enumerate(copies):

                @pl.when(which == one)
                def _():
                    other.start()
                    mine.start()

        chunks(t, RUN, one)

    def arrived(i):
        _, copies = raw(i)
        copies[0][0].wait()
        copies[0][1].wait_recv()

    def passes(i, o, rightward):
        s, e = lax.rem(i, S_OUT), lax.rem(i, S_IN)
        if rightward:
            return remote(rout.at[s, o - 1], rin.at[e, o - 1], rs.at[s, o], rr.at[e, o], right)
        return remote(lout.at[s, o], lin.at[e, o], ls.at[s, o], lr.at[e, o], left)

    def passing(t, rightward):
        if rightward:
            before, box, out = z, rin, rout
            many, has_in, first = CHIPS - 1 - z, z > 0, z <= 1
        else:
            before, box, out = CHIPS - 1 - z, lin, lout
            many, has_in, first = z, z < CHIPS - 1, z > 1
        now = t - LAG - HOP * before

        @pl.when(first)
        def _():
            chunks(now, RUN, arrived)

        def lane(k, _):
            o = CHIPS - 1 - k if rightward else k
            slot = o - 1 if rightward else o

            def one(i):
                raw_slot, in_slot, out_slot = lax.rem(i, S_RAW), lax.rem(i, S_IN), lax.rem(i, S_OUT)
                copy = passes(i, o, rightward)

                @pl.when(i >= S_OUT)
                def _():
                    copy.wait_send()

                @pl.when(has_in)
                def _():
                    copy.wait_recv()

                    def add(rows):
                        so_far = f32(own.at[raw_slot, o, rows]) + f32(sib.at[raw_slot, o, rows])
                        out[out_slot, slot, rows] = (so_far + f32(box.at[in_slot, slot, rows])).astype(jnp.bfloat16)

                    pieces(add)

                @pl.when(jnp.logical_not(has_in))
                def _():
                    def add(rows):
                        so_far = f32(own.at[raw_slot, o, rows]) + f32(sib.at[raw_slot, o, rows])
                        out[out_slot, slot, rows] = so_far.astype(jnp.bfloat16)

                    pieces(add)

                copy.start()

            chunks(now, jnp.minimum(CHIPS - 2 - k, RUN), one)
            return 0

        lax.fori_loop(0, many, lane, 0)

    def loads(i):
        which, layer, rows = place(i)
        s = lax.rem(i, S_ADAM)
        return which, [
            (
                pltpu.make_async_copy(m[one].at[layer, rows], new_m.at[one, layer, rows], ld_sem.at[s, 0]),
                pltpu.make_async_copy(v[one].at[layer, rows], new_v.at[one, layer, rows], ld_sem.at[s, 1]),
                pltpu.make_async_copy(w[one].at[layer, d, rows], wi.at[s], ld_sem.at[s, 2]),
            )
            for one in range(3)
        ]

    def fetch_state(t):
        i = t - turn(z) + S_ADAM - 1

        @pl.when(inside(i))
        def _():
            which, copies = loads(i)
            for one, each in enumerate(copies):

                @pl.when(which == one)
                def _():
                    for copy in each:
                        copy.start()

    def stores(i, there):
        s, a = lax.rem(i, S_ADAM), lax.rem(i, S_AG)
        local = pltpu.make_async_copy(wo.at[s], there, st_sem.at[s])
        to_right = remote(wo.at[s], there, own_s.at[s, 0], ag_r.at[a, z], right)
        to_left = remote(wo.at[s], there, own_s.at[s, 1], ag_r.at[a, z], left)
        to_twin = remote(wo.at[s], there, own_s.at[s, 2], sib_r.at[a, z], twin)
        return local, to_right, to_left, to_twin

    def stored(i):
        local, to_right, to_left, to_twin = stores(i, block_sized)

        @pl.when((i < kept) | (i >= early))
        def _():
            local.wait()

        to_twin.wait_send()

        @pl.when((i < early) & (z < CHIPS - 1))
        def _():
            to_right.wait_send()

        @pl.when((i < early) & (z > 0))
        def _():
            to_left.wait_send()

    def adam(t):
        i = t - turn(z)

        @pl.when(inside(i))
        def _():
            raw_slot, in_slot, s = lax.rem(i, S_RAW), lax.rem(i, S_IN), lax.rem(i, S_ADAM)
            _, copies = loads(i)
            for copy in copies[0]:
                copy.wait()

            raw(i)[1][0][1].wait_send()

            @pl.when(i >= S_ADAM)
            def _():
                stored(i - S_ADAM)

            @pl.when(z > 0)
            def _():
                passes(i, z, True).wait_recv()

            @pl.when(z < CHIPS - 1)
            def _():
                passes(i, z, False).wait_recv()

            def add(boxes):
                def one(rows):
                    so_far = f32(own.at[raw_slot, z, rows]) + f32(sib.at[raw_slot, z, rows])
                    for box, lane in boxes:
                        so_far += f32(box.at[in_slot, lane, rows])
                    total[rows] = so_far

                pieces(one)

            for here, boxes in ((z == 0, [(lin, z)]), (z == CHIPS - 1, [(rin, z - 1)]), ((z > 0) & (z < CHIPS - 1), [(rin, z - 1), (lin, z)])):

                @pl.when(here)
                def _(boxes=boxes):
                    add(boxes)

            which, layer, base = place(i)

            def step(rows):
                to = pl.ds(pl.multiple_of(base.start + rows.start, 8), PIECE)
                grad = total[rows].astype(jnp.bfloat16).astype(jnp.float32)
                m1 = 0.9 * new_m[which, layer, to] + 0.1 * grad
                v1 = 0.95 * new_v[which, layer, to] + 0.05 * grad * grad
                w0 = f32(wi.at[s, rows])
                new_m[which, layer, to] = m1
                new_v[which, layer, to] = v1
                wo[s, rows] = (w0 - 0.02 * (m1 * lax.rsqrt(v1 + 1e-8) + 0.1 * w0)).astype(jnp.bfloat16)

            pieces(step)

            @pl.when((i >= kept) & (i < early))
            def _():
                def keep(rows):
                    at = (i - kept) * rows_per + rows.start
                    last_w[d, pl.ds(pl.multiple_of(at, 8), PIECE)] = wo[s, rows]

                pieces(keep)

            @pl.when(i >= early)
            def _():
                stores(i, late_w.at[i - early])[0].start()
                stores(i, late_twin.at[i - early])[3].start()

            for here, there in spots(i, d):

                @pl.when(here & (i < early))
                def _(there=there):
                    local, to_right, to_left, to_twin = stores(i, there)

                    @pl.when(z < CHIPS - 1)
                    def _():
                        to_right.start()

                    @pl.when(z > 0)
                    def _():
                        to_left.start()

                    to_twin.start()
                    if there.memory_space != pltpu.VMEM:
                        local.start()

    def forwards(i, o, to, there):
        a = lax.rem(i, S_AG)
        return remote(there, there, fwd_s.at[a, o], ag_r.at[a, o], to), remote(there, there, sib_s.at[a, o], sib_r.at[a, o], twin)

    def sent(i, o, to, on):
        ahead, across = forwards(i, o, to, block_sized)

        @pl.when(on)
        def _():
            ahead.wait_send()

        across.wait_send()

    def gathering(t, rightward):
        many, to, on = (z, right, z < CHIPS - 1) if rightward else (CHIPS - 1 - z, left, z > 0)

        def lane(k, _):
            o = z - 1 - k if rightward else z + 1 + k
            i = t - turn(o) - HOP2 * (k + 1)

            @pl.when((i >= SENT) & (i < early + SENT))
            def _():
                sent(i - SENT, o, to, on)

            @pl.when((i >= 0) & (i < early))
            def _():
                forwards(i, o, to, block_sized)[0].wait_recv()
                for here, there in spots(i, o * 2 + c):

                    @pl.when(here)
                    def _(there=there):
                        ahead, across = forwards(i, o, to, there)

                        @pl.when(on)
                        def _():
                            ahead.start()

                        across.start()

            return 0

        lax.fori_loop(0, many, lane, 0)

    def crossing(t):
        def lane(o, _):
            i = t - turn(o) - HOP2 * jnp.abs(z - o) - 2

            @pl.when((i >= 0) & (i < early))
            def _():
                forwards(i, o, right, block_sized)[1].wait_recv()

            return 0

        lax.fori_loop(0, CHIPS, lane, 0)

    def step(t, _):
        passing(t, True)
        passing(t, False)
        adam(t)
        gathering(t, True)
        gathering(t, False)
        fetch(t)
        fetch_state(t)
        crossing(t)
        return 0

    lax.fori_loop(0, LAG + HOP * (CHIPS - 1) + max(n, early + HOP2 * (CHIPS - 1) + max(2, SENT)), step, 0)

    def pass_left(k, _):
        def to_right(o, _):
            passes(n - S_OUT + k, o, True).wait_send()
            return 0

        def to_left(o, _):
            passes(n - S_OUT + k, o, False).wait_send()
            return 0

        lax.fori_loop(z + 1, CHIPS, to_right, 0)
        lax.fori_loop(0, z, to_left, 0)
        return 0

    lax.fori_loop(0, S_OUT, pass_left, 0)

    def stores_left(k, _):
        stored(n - S_ADAM + k)
        return 0

    lax.fori_loop(0, S_ADAM, stores_left, 0)

    def late_left(k, _):
        forwards(early + k, z, right, block_sized)[1].wait_recv()
        return 0

    lax.fori_loop(0, LATE, late_left, 0)


def write_out(through, straight, held, in_sem, out_sem, sem):
    n, ahead = len(through), S_COPY - 4
    assert n >= S_COPY

    def slot(j):
        return held.at[j % S_COPY, pl.ds(0, through[j][0].shape[0])]

    def load(j):
        return pltpu.make_async_copy(through[j][0], slot(j), in_sem.at[j % S_COPY])

    def store(j):
        return pltpu.make_async_copy(slot(j), through[j][1], out_sem.at[j % S_COPY])

    rest = [pltpu.make_async_copy(*pair, sem.at[k]) for k, pair in enumerate(straight)]
    for j in range(ahead):
        load(j).start()
    for j in range(n):
        load(j).wait()
        store(j).start()
        if j + ahead < n:
            if j + ahead >= S_COPY:
                store(j + ahead - S_COPY).wait()
            load(j + ahead).start()
    for copy in rest:
        copy.start()
    for j in range(n - S_COPY, n):
        store(j).wait()
    for copy in rest:
        copy.wait()


def spans(source, target, rows):
    many = source.shape[0]
    return [(source.at[pl.ds(p, min(rows, many - p))], target.at[pl.ds(p, min(rows, many - p))]) for p in range(0, many, rows)]


def write_most(new_w, last_w, state, *refs):
    outs, (held, *sems) = refs[:9], refs[9:]
    layers, owners, block, _ = outs[2].shape
    more = MORE * TILES * 8
    through = []
    for k in range(2):
        for layer in range(layers):
            there = pl.ds(0, block - more if (k, layer) == (1, layers - 1) else block)
            for owner in range(owners):
                through += spans(new_w.at[k, layer, owner, there], outs[k].at[layer, owner, there], held.shape[1])
    straight = [(last_w.at[:, pl.ds(0, more)], outs[1].at[layers - 1, :, pl.ds(block - more, more)])]
    straight += [(last_w.at[:, pl.ds(more + layer * block, block)], outs[2].at[layer]) for layer in range(layers - 1)]
    straight += [(state.at[k // 3, k % 3], outs[3 + k]) for k in range(6)]
    write_out(through, straight, held, *sems)


def write_last(so_far, last_w, out, sem):
    del so_far
    layers, _, block, _ = out.shape
    done = (layers - 1) * block + MORE * TILES * 8
    rest = last_w.shape[1] - done
    copy = pltpu.make_async_copy(last_w.at[:, pl.ds(done, rest)], out.at[layers - 1, :, pl.ds(0, rest)], sem)
    copy.start()
    copy.wait()


def write_late(so_far, *refs):
    del so_far
    blocks, (out, sem) = refs[: 2 * CHIPS], refs[2 * CHIPS :]
    d = lax.axis_index("dp")
    z, c = lax.div(d, 2), lax.rem(d, 2)
    rows = blocks[0].shape[0]
    copies = []
    for k, block in enumerate(blocks):
        owner = lax.rem(z + AWAY[k % CHIPS], CHIPS) * 2 + (c if k < CHIPS else 1 - c)
        copies.append(pltpu.make_async_copy(block, out.at[out.shape[0] - 1, owner, pl.ds(out.shape[2] - rows, rows)], sem.at[k]))
    for copy in copies:
        copy.start()
    for copy in copies:
        copy.wait()


def solution(mesh):
    bf16, f32 = jnp.bfloat16, jnp.float32

    def step(*arrays):
        terms, weights, m, v = (arrays[i : i + 3] for i in (0, 3, 6, 9))
        layers = weights[0].shape[0]
        block = weights[0].shape[1] * weights[0].shape[2] // (2 * CHIPS * 128)
        rows = TILES * 8
        args = [tiles(t[0]).reshape(layers, CHIPS, 2, block, 128) for t in terms]
        args += [tiles(w).reshape(layers, 2 * CHIPS, block, 128) for w in weights]
        args += [tiles(x) for x in (*m, *v)]
        dma = pltpu.SemaphoreType.DMA
        in_hbm, in_vmem = pl.BlockSpec(memory_space=pltpu.HBM), pl.BlockSpec(memory_space=pltpu.VMEM)
        new_w, last_w, late_w, late_twin, state = pl.pallas_call(
            functools.partial(kernel, block // rows, layers),
            out_shape=[
                jax.ShapeDtypeStruct((2, layers, 2 * CHIPS, block, 128), bf16),
                pltpu.VMEM((2 * CHIPS, layers * block + (MORE - LATE) * rows, 128), bf16),
                jax.ShapeDtypeStruct((LATE, rows, 128), bf16),
                jax.ShapeDtypeStruct((LATE, rows, 128), bf16),
                pltpu.VMEM((2, 3, layers, block, 128), f32),
            ],
            in_specs=[in_hbm] * 12,
            out_specs=[in_hbm, in_vmem, in_hbm, in_hbm, in_vmem],
            scratch_shapes=[
                pltpu.VMEM((S_RAW, CHIPS, rows, 128), bf16),
                pltpu.VMEM((S_RAW, CHIPS, rows, 128), bf16),
                pltpu.VMEM((S_IN, CHIPS - 1, rows, 128), bf16),
                pltpu.VMEM((S_IN, CHIPS - 1, rows, 128), bf16),
                pltpu.VMEM((S_OUT, CHIPS - 1, rows, 128), bf16),
                pltpu.VMEM((S_OUT, CHIPS - 1, rows, 128), bf16),
                pltpu.VMEM((rows, 128), f32),
                pltpu.VMEM((S_ADAM, rows, 128), bf16),
                pltpu.VMEM((S_ADAM, rows, 128), bf16),
                dma((S_RAW,)),
                dma((S_RAW,)),
                dma((S_RAW,)),
                dma((S_OUT, CHIPS)),
                dma((S_IN, CHIPS)),
                dma((S_OUT, CHIPS)),
                dma((S_IN, CHIPS)),
                dma((S_ADAM, 3)),
                dma((S_ADAM,)),
                dma((S_ADAM, 3)),
                dma((S_AG, CHIPS)),
                dma((S_AG, CHIPS)),
                dma((S_AG, CHIPS)),
                dma((S_AG, CHIPS)),
            ],
            compiler_params=pltpu.CompilerParams(collective_id=0, has_side_effects=True, vmem_limit_bytes=ROOM),
        )(*(pltpu.with_memory_space_constraint(x, pltpu.HBM) for x in args))
        last_w, state = (pltpu.with_memory_space_constraint(x, pltpu.VMEM) for x in (last_w, state))
        every = range(2 * CHIPS)
        every = range(2 * CHIPS)
        late = [late_w.reshape(LATE * rows, 128)]
        late += [lax.ppermute(late[0], "dp", [((d + 2 * k) % (2 * CHIPS), d) for d in every]) for k in AWAY[1:]]
        grant = pltpu.CompilerParams(vmem_limit_bytes=ROOM)
        most = pl.pallas_call(
            write_most,
            out_shape=[jax.ShapeDtypeStruct((layers, 2 * CHIPS, block, 128), bf16)] * 3 + [jax.ShapeDtypeStruct((layers, block, 128), f32)] * 6,
            in_specs=[in_hbm, in_vmem, in_vmem],
            out_specs=[in_hbm] * 9,
            scratch_shapes=[pltpu.VMEM((S_COPY, SPAN, 128), bf16), dma((S_COPY,)), dma((S_COPY,)), dma((6 + layers,))],
            compiler_params=grant,
            cost_estimate=pl.CostEstimate(flops=MOST_COST, bytes_accessed=150 * 10**6, transcendentals=0),
        )(new_w, last_w, state)
        twins = [late_twin.reshape(LATE * rows, 128)]
        twins += [lax.ppermute(x, "dp", [(d, d ^ 1) for d in every]) for x in late[1:]]
        last = pl.pallas_call(
            write_last,
            out_shape=jax.ShapeDtypeStruct(most[2].shape, bf16),
            in_specs=[in_hbm, in_vmem],
            out_specs=in_hbm,
            scratch_shapes=[dma],
            input_output_aliases={0: 0},
            compiler_params=grant,
            cost_estimate=pl.CostEstimate(flops=MOST_COST // 16, bytes_accessed=7 * 10**6, transcendentals=0),
        )(most[2], last_w)
        last = pl.pallas_call(
            write_late,
            out_shape=jax.ShapeDtypeStruct(last.shape, bf16),
            in_specs=[in_hbm] + [in_vmem] * (2 * CHIPS),
            out_specs=in_hbm,
            scratch_shapes=[dma((2 * CHIPS,))],
            input_output_aliases={0: 0},
            compiler_params=grant,
        )(last, *late, *twins)
        outs = [*(x.reshape(layers, -1, 128) for x in (most[0], most[1], last)), *most[3:]]
        outs = [untiles(o, *old.shape[1:]) for o, old in zip(outs, (*weights, *m, *v), strict=True)]
        return tuple(outs)

    all_of, cut = P(None, None, None), P(None, "dp", None)
    return jax.shard_map(
        step,
        mesh=mesh,
        in_specs=(P(("rep", "dp"), None, None, None),) * 3 + (all_of,) * 3 + (cut,) * 6,
        out_specs=(P("rep", None, None),) * 3 + (P("rep", "dp", None),) * 6,
        check_vma=False,
    )
```

```python
import functools

import jax
import jax.numpy as jnp
from jax import lax
from jax.experimental import pallas as pl
from jax.experimental.pallas import tpu as pltpu
from jax.sharding import PartitionSpec as P

MESH = pl.DeviceIdType.MESH
CHIPS = 4
TILES = 35
HOP = 1
HOP2 = 1
RUN = 2
LAG = 2
S_RAW, S_IN, S_OUT, S_ADAM, S_AG = 9, 7, 2, 3, 16
SENT = 5
MORE = 3
LATE = 7
ROOM = 9728 * 1024
SPAN, S_COPY = 1400, 24
MOST_COST = 10**11
AWAY = 0, 1, 3, 2
PIECE = 40


def tiles(x):
    *lead, r, c = x.shape
    return x.reshape(*lead, r // 8, 8, c // 128, 128).swapaxes(-3, -2).reshape(*lead, r * c // 128, 128)


def untiles(x, r, c):
    lead = x.shape[:-2]
    return x.reshape(*lead, r // 8, c // 128, 8, 128).swapaxes(-3, -2).reshape(*lead, r, c)


def kernel(
    per_layer, layers, *refs
):
    g, w, m, v = (refs[i : i + 3] for i in (0, 3, 6, 9))
    new_w, last_w, late_w, late_twin, state = refs[12:17]
    new_m, new_v = state.at[0], state.at[1]
    own, sib, rin, lin, rout, lout, total, wi, wo = refs[17:26]
    own_sem, raw_s, raw_r, rs, rr, ls, lr, ld_sem, st_sem, own_s, fwd_s, ag_r, sib_s, sib_r = refs[26:]
    rows_per = TILES * 8
    n = len(g) * layers * per_layer
    early = n - LATE
    kept = n - layers * per_layer - MORE
    d = lax.axis_index("dp")
    z, c = lax.div(d, 2), lax.rem(d, 2)
    right, left, twin = {"dp": lax.rem(d + 2, 8)}, {"dp": lax.rem(d + 6, 8)}, {"dp": z * 2 + 1 - c}
    far = jnp.maximum(z, CHIPS - 1 - z)

    def turn(o):
        return LAG + HOP * jnp.maximum(o, CHIPS - 1 - o)

    def place(i):
        which, rest = lax.div(i, layers * per_layer), lax.rem(i, layers * per_layer)
        layer, k = lax.div(rest, per_layer), lax.rem(rest, per_layer)
        return which, layer, pl.ds(pl.multiple_of(k * rows_per, 8), rows_per)

    def spots(i, owner):
        which, layer, rows = place(i)
        at = pl.ds(pl.multiple_of((i - kept) * rows_per, 8), rows_per)
        return (i < kept, new_w.at[which, layer, owner, rows]), (i >= kept, last_w.at[owner, at])

    block_sized = new_w.at[0, 0, 0, pl.ds(0, rows_per)]

    def inside(i):
        return (i >= 0) & (i < n)

    def remote(src, dst, s, r, to):
        return pltpu.make_async_remote_copy(src, dst, s, r, device_id=to, device_id_type=MESH)

    def pieces(body):
        def one(p, _):
            body(pl.ds(pl.multiple_of(p * PIECE, 8), PIECE))
            return 0

        lax.fori_loop(0, rows_per // PIECE, one, 0)

    def f32(ref):
        return ref[...].astype(jnp.float32)

    barrier = pltpu.get_barrier_semaphore()

    @pl.when(z < CHIPS - 1)
    def _():
        pl.semaphore_signal(barrier, 1, device_id=right, device_id_type=MESH)

    @pl.when(z > 0)
    def _():
        pl.semaphore_signal(barrier, 1, device_id=left, device_id_type=MESH)

    pl.semaphore_signal(barrier, 1, device_id=twin, device_id_type=MESH)
    pl.semaphore_wait(barrier, 1 + (z > 0).astype(jnp.int32) + (z < CHIPS - 1).astype(jnp.int32))

    def raw(i):
        which, layer, rows = place(i)
        s = lax.rem(i, S_RAW)
        return which, [
            (
                pltpu.make_async_copy(one.at[layer, :, c, rows], own.at[s], own_sem.at[s]),
                remote(one.at[layer, :, 1 - c, rows], sib.at[s], raw_s.at[s], raw_r.at[s], twin),
            )
            for one in g
        ]

    def chunks(step, ahead, body):
        def upto(x):
            return jnp.clip(jnp.minimum(2 * x, x + ahead), 0, n)

        def one(i, _):
            body(i)
            return 0

        lax.fori_loop(upto(step), upto(step + 1), one, 0)

    def fetch(t):
        def one(i):
            which, copies = raw(i)
            for one, (mine, other) in enumerate(copies):

                @pl.when(which == one)
                def _():
                    other.start()
                    mine.start()

        chunks(t, RUN, one)

    def arrived(i):
        _, copies = raw(i)
        copies[0][0].wait()
        copies[0][1].wait_recv()

    def passes(i, o, rightward):
        s, e = lax.rem(i, S_OUT), lax.rem(i, S_IN)
        if rightward:
            return remote(rout.at[s, o - 1], rin.at[e, o - 1], rs.at[s, o], rr.at[e, o], right)
        return remote(lout.at[s, o], lin.at[e, o], ls.at[s, o], lr.at[e, o], left)

    def passing(t, rightward):
        if rightward:
            before, box, out = z, rin, rout
            many, has_in, first = CHIPS - 1 - z, z > 0, z <= 1
        else:
            before, box, out = CHIPS - 1 - z, lin, lout
            many, has_in, first = z, z < CHIPS - 1, z > 1
        now = t - LAG - HOP * before

        @pl.when(first)
        def _():
            chunks(now, RUN, arrived)

        def lane(k, _):
            o = CHIPS - 1 - k if rightward else k
            slot = o - 1 if rightward else o

            def one(i):
                raw_slot, in_slot, out_slot = lax.rem(i, S_RAW), lax.rem(i, S_IN), lax.rem(i, S_OUT)
                copy = passes(i, o, rightward)

                @pl.when(i >= S_OUT)
                def _():
                    copy.wait_send()

                @pl.when(has_in)
                def _():
                    copy.wait_recv()

                    def add(rows):
                        so_far = f32(own.at[raw_slot, o, rows]) + f32(sib.at[raw_slot, o, rows])
                        out[out_slot, slot, rows] = (so_far + f32(box.at[in_slot, slot, rows])).astype(jnp.bfloat16)

                    pieces(add)

                @pl.when(jnp.logical_not(has_in))
                def _():
                    def add(rows):
                        so_far = f32(own.at[raw_slot, o, rows]) + f32(sib.at[raw_slot, o, rows])
                        out[out_slot, slot, rows] = so_far.astype(jnp.bfloat16)

                    pieces(add)

                copy.start()

            chunks(now, jnp.minimum(CHIPS - 2 - k, RUN), one)
            return 0

        lax.fori_loop(0, many, lane, 0)

    def loads(i):
        which, layer, rows = place(i)
        s = lax.rem(i, S_ADAM)
        return which, [
            (
                pltpu.make_async_copy(m[one].at[layer, rows], new_m.at[one, layer, rows], ld_sem.at[s, 0]),
                pltpu.make_async_copy(v[one].at[layer, rows], new_v.at[one, layer, rows], ld_sem.at[s, 1]),
                pltpu.make_async_copy(w[one].at[layer, d, rows], wi.at[s], ld_sem.at[s, 2]),
            )
            for one in range(3)
        ]

    def fetch_state(t):
        i = t - turn(z) + S_ADAM - 1

        @pl.when(inside(i))
        def _():
            which, copies = loads(i)
            for one, each in enumerate(copies):

                @pl.when(which == one)
                def _():
                    for copy in each:
                        copy.start()

    def stores(i, there):
        s, a = lax.rem(i, S_ADAM), lax.rem(i, S_AG)
        local = pltpu.make_async_copy(wo.at[s], there, st_sem.at[s])
        to_right = remote(wo.at[s], there, own_s.at[s, 0], ag_r.at[a, z], right)
        to_left = remote(wo.at[s], there, own_s.at[s, 1], ag_r.at[a, z], left)
        to_twin = remote(wo.at[s], there, own_s.at[s, 2], sib_r.at[a, z], twin)
        return local, to_right, to_left, to_twin

    def stored(i):
        local, to_right, to_left, to_twin = stores(i, block_sized)

        @pl.when((i < kept) | (i >= early))
        def _():
            local.wait()

        to_twin.wait_send()

        @pl.when((i < early) & (z < CHIPS - 1))
        def _():
            to_right.wait_send()

        @pl.when((i < early) & (z > 0))
        def _():
            to_left.wait_send()

    def adam(t):
        i = t - turn(z)

        @pl.when(inside(i))
        def _():
            raw_slot, in_slot, s = lax.rem(i, S_RAW), lax.rem(i, S_IN), lax.rem(i, S_ADAM)
            _, copies = loads(i)
            for copy in copies[0]:
                copy.wait()

            raw(i)[1][0][1].wait_send()

            @pl.when(i >= S_ADAM)
            def _():
                stored(i - S_ADAM)

            @pl.when(z > 0)
            def _():
                passes(i, z, True).wait_recv()

            @pl.when(z < CHIPS - 1)
            def _():
                passes(i, z, False).wait_recv()

            def add(boxes):
                def one(rows):
                    so_far = f32(own.at[raw_slot, z, rows]) + f32(sib.at[raw_slot, z, rows])
                    for box, lane in boxes:
                        so_far += f32(box.at[in_slot, lane, rows])
                    total[rows] = so_far

                pieces(one)

            for here, boxes in ((z == 0, [(lin, z)]), (z == CHIPS - 1, [(rin, z - 1)]), ((z > 0) & (z < CHIPS - 1), [(rin, z - 1), (lin, z)])):

                @pl.when(here)
                def _(boxes=boxes):
                    add(boxes)

            which, layer, base = place(i)

            def step(rows):
                to = pl.ds(pl.multiple_of(base.start + rows.start, 8), PIECE)
                grad = total[rows].astype(jnp.bfloat16).astype(jnp.float32)
                m1 = 0.9 * new_m[which, layer, to] + 0.1 * grad
                v1 = 0.95 * new_v[which, layer, to] + 0.05 * grad * grad
                w0 = f32(wi.at[s, rows])
                new_m[which, layer, to] = m1
                new_v[which, layer, to] = v1
                wo[s, rows] = (w0 - 0.02 * (m1 * lax.rsqrt(v1 + 1e-8) + 0.1 * w0)).astype(jnp.bfloat16)

            pieces(step)

            @pl.when((i >= kept) & (i < early))
            def _():
                def keep(rows):
                    at = (i - kept) * rows_per + rows.start
                    last_w[d, pl.ds(pl.multiple_of(at, 8), PIECE)] = wo[s, rows]

                pieces(keep)

            @pl.when(i >= early)
            def _():
                stores(i, late_w.at[i - early])[0].start()
                stores(i, late_twin.at[i - early])[3].start()

            for here, there in spots(i, d):

                @pl.when(here & (i < early))
                def _(there=there):
                    local, to_right, to_left, to_twin = stores(i, there)

                    @pl.when(z < CHIPS - 1)
                    def _():
                        to_right.start()

                    @pl.when(z > 0)
                    def _():
                        to_left.start()

                    to_twin.start()
                    if there.memory_space != pltpu.VMEM:
                        local.start()

    def forwards(i, o, to, there):
        a = lax.rem(i, S_AG)
        return remote(there, there, fwd_s.at[a, o], ag_r.at[a, o], to), remote(there, there, sib_s.at[a, o], sib_r.at[a, o], twin)

    def sent(i, o, to, on):
        ahead, across = forwards(i, o, to, block_sized)

        @pl.when(on)
        def _():
            ahead.wait_send()

        across.wait_send()

    def gathering(t, rightward):
        many, to, on = (z, right, z < CHIPS - 1) if rightward else (CHIPS - 1 - z, left, z > 0)

        def lane(k, _):
            o = z - 1 - k if rightward else z + 1 + k
            i = t - turn(o) - HOP2 * (k + 1)

            @pl.when((i >= SENT) & (i < early + SENT))
            def _():
                sent(i - SENT, o, to, on)

            @pl.when((i >= 0) & (i < early))
            def _():
                forwards(i, o, to, block_sized)[0].wait_recv()
                for here, there in spots(i, o * 2 + c):

                    @pl.when(here)
                    def _(there=there):
                        ahead, across = forwards(i, o, to, there)

                        @pl.when(on)
                        def _():
                            ahead.start()

                        across.start()

            return 0

        lax.fori_loop(0, many, lane, 0)

    def crossing(t):
        def lane(o, _):
            i = t - turn(o) - HOP2 * jnp.abs(z - o) - 2

            @pl.when((i >= 0) & (i < early))
            def _():
                forwards(i, o, right, block_sized)[1].wait_recv()

            return 0

        lax.fori_loop(0, CHIPS, lane, 0)

    def step(t, _):
        passing(t, True)
        passing(t, False)
        adam(t)
        gathering(t, True)
        gathering(t, False)
        fetch(t)
        fetch_state(t)
        crossing(t)
        return 0

    lax.fori_loop(0, LAG + HOP * (CHIPS - 1) + max(n, early + HOP2 * (CHIPS - 1) + max(2, SENT)), step, 0)

    def pass_left(k, _):
        def to_right(o, _):
            passes(n - S_OUT + k, o, True).wait_send()
            return 0

        def to_left(o, _):
            passes(n - S_OUT + k, o, False).wait_send()
            return 0

        lax.fori_loop(z + 1, CHIPS, to_right, 0)
        lax.fori_loop(0, z, to_left, 0)
        return 0

    lax.fori_loop(0, S_OUT, pass_left, 0)

    def stores_left(k, _):
        stored(n - S_ADAM + k)
        return 0

    lax.fori_loop(0, S_ADAM, stores_left, 0)

    def late_left(k, _):
        forwards(early + k, z, right, block_sized)[1].wait_recv()
        return 0

    lax.fori_loop(0, LATE, late_left, 0)


def write_out(through, straight, held, in_sem, out_sem, sem):
    n, ahead = len(through), S_COPY - 4
    assert n >= S_COPY

    def slot(j):
        return held.at[j % S_COPY, pl.ds(0, through[j][0].shape[0])]

    def load(j):
        return pltpu.make_async_copy(through[j][0], slot(j), in_sem.at[j % S_COPY])

    def store(j):
        return pltpu.make_async_copy(slot(j), through[j][1], out_sem.at[j % S_COPY])

    rest = [pltpu.make_async_copy(*pair, sem.at[k]) for k, pair in enumerate(straight)]
    for j in range(ahead):
        load(j).start()
    for j in range(n):
        load(j).wait()
        store(j).start()
        if j + ahead < n:
            if j + ahead >= S_COPY:
                store(j + ahead - S_COPY).wait()
            load(j + ahead).start()
    for copy in rest:
        copy.start()
    for j in range(n - S_COPY, n):
        store(j).wait()
    for copy in rest:
        copy.wait()


def spans(source, target, rows):
    many = source.shape[0]
    return [(source.at[pl.ds(p, min(rows, many - p))], target.at[pl.ds(p, min(rows, many - p))]) for p in range(0, many, rows)]


def write_most(new_w, last_w, state, *refs):
    outs, (held, *sems) = refs[:9], refs[9:]
    layers, owners, block, _ = outs[2].shape
    more = MORE * TILES * 8
    through = []
    for k in range(2):
        for layer in range(layers):
            there = pl.ds(0, block - more if (k, layer) == (1, layers - 1) else block)
            for owner in range(owners):
                through += spans(new_w.at[k, layer, owner, there], outs[k].at[layer, owner, there], held.shape[1])
    straight = [(last_w.at[:, pl.ds(0, more)], outs[1].at[layers - 1, :, pl.ds(block - more, more)])]
    straight += [(last_w.at[:, pl.ds(more + layer * block, block)], outs[2].at[layer]) for layer in range(layers - 1)]
    straight += [(state.at[k // 3, k % 3], outs[3 + k]) for k in range(6)]
    write_out(through, straight, held, *sems)


def write_last(so_far, last_w, out, sem):
    del so_far
    layers, _, block, _ = out.shape
    done = (layers - 1) * block + MORE * TILES * 8
    rest = last_w.shape[1] - done
    copy = pltpu.make_async_copy(last_w.at[:, pl.ds(done, rest)], out.at[layers - 1, :, pl.ds(0, rest)], sem)
    copy.start()
    copy.wait()


def write_late(so_far, *refs):
    del so_far
    blocks, (out, sem) = refs[: 2 * CHIPS], refs[2 * CHIPS :]
    d = lax.axis_index("dp")
    z, c = lax.div(d, 2), lax.rem(d, 2)
    rows = blocks[0].shape[0]
    copies = []
    for k, block in enumerate(blocks):
        owner = lax.rem(z + AWAY[k % CHIPS], CHIPS) * 2 + (c if k < CHIPS else 1 - c)
        copies.append(pltpu.make_async_copy(block, out.at[out.shape[0] - 1, owner, pl.ds(out.shape[2] - rows, rows)], sem.at[k]))
    for copy in copies:
        copy.start()
    for copy in copies:
        copy.wait()


def solution(mesh):
    bf16, f32 = jnp.bfloat16, jnp.float32

    def step(*arrays):
        terms, weights, m, v = (arrays[i : i + 3] for i in (0, 3, 6, 9))
        layers = weights[0].shape[0]
        block = weights[0].shape[1] * weights[0].shape[2] // (2 * CHIPS * 128)
        rows = TILES * 8
        args = [tiles(t[0]).reshape(layers, CHIPS, 2, block, 128) for t in terms]
        args += [tiles(w).reshape(layers, 2 * CHIPS, block, 128) for w in weights]
        args += [tiles(x) for x in (*m, *v)]
        dma = pltpu.SemaphoreType.DMA
        in_hbm, in_vmem = pl.BlockSpec(memory_space=pltpu.HBM), pl.BlockSpec(memory_space=pltpu.VMEM)
        new_w, last_w, late_w, late_twin, state = pl.pallas_call(
            functools.partial(kernel, block // rows, layers),
            out_shape=[
                jax.ShapeDtypeStruct((2, layers, 2 * CHIPS, block, 128), bf16),
                pltpu.VMEM((2 * CHIPS, layers * block + (MORE - LATE) * rows, 128), bf16),
                jax.ShapeDtypeStruct((LATE, rows, 128), bf16),
                jax.ShapeDtypeStruct((LATE, rows, 128), bf16),
                pltpu.VMEM((2, 3, layers, block, 128), f32),
            ],
            in_specs=[in_hbm] * 12,
            out_specs=[in_hbm, in_vmem, in_hbm, in_hbm, in_vmem],
            scratch_shapes=[
                pltpu.VMEM((S_RAW, CHIPS, rows, 128), bf16),
                pltpu.VMEM((S_RAW, CHIPS, rows, 128), bf16),
                pltpu.VMEM((S_IN, CHIPS - 1, rows, 128), bf16),
                pltpu.VMEM((S_IN, CHIPS - 1, rows, 128), bf16),
                pltpu.VMEM((S_OUT, CHIPS - 1, rows, 128), bf16),
                pltpu.VMEM((S_OUT, CHIPS - 1, rows, 128), bf16),
                pltpu.VMEM((rows, 128), f32),
                pltpu.VMEM((S_ADAM, rows, 128), bf16),
                pltpu.VMEM((S_ADAM, rows, 128), bf16),
                dma((S_RAW,)),
                dma((S_RAW,)),
                dma((S_RAW,)),
                dma((S_OUT, CHIPS)),
                dma((S_IN, CHIPS)),
                dma((S_OUT, CHIPS)),
                dma((S_IN, CHIPS)),
                dma((S_ADAM, 3)),
                dma((S_ADAM,)),
                dma((S_ADAM, 3)),
                dma((S_AG, CHIPS)),
                dma((S_AG, CHIPS)),
                dma((S_AG, CHIPS)),
                dma((S_AG, CHIPS)),
            ],
            compiler_params=pltpu.CompilerParams(collective_id=0, has_side_effects=True, vmem_limit_bytes=ROOM),
        )(*(pltpu.with_memory_space_constraint(x, pltpu.HBM) for x in args))
        last_w, state = (pltpu.with_memory_space_constraint(x, pltpu.VMEM) for x in (last_w, state))
        every = range(2 * CHIPS)
        every = range(2 * CHIPS)
        late = [late_w.reshape(LATE * rows, 128)]
        late += [lax.ppermute(late[0], "dp", [((d + 2 * k) % (2 * CHIPS), d) for d in every]) for k in AWAY[1:]]
        grant = pltpu.CompilerParams(vmem_limit_bytes=ROOM)
        most = pl.pallas_call(
            write_most,
            out_shape=[jax.ShapeDtypeStruct((layers, 2 * CHIPS, block, 128), bf16)] * 3 + [jax.ShapeDtypeStruct((layers, block, 128), f32)] * 6,
            in_specs=[in_hbm, in_vmem, in_vmem],
            out_specs=[in_hbm] * 9,
            scratch_shapes=[pltpu.VMEM((S_COPY, SPAN, 128), bf16), dma((S_COPY,)), dma((S_COPY,)), dma((6 + layers,))],
            compiler_params=grant,
            cost_estimate=pl.CostEstimate(flops=MOST_COST, bytes_accessed=150 * 10**6, transcendentals=0),
        )(new_w, last_w, state)
        twins = [late_twin.reshape(LATE * rows, 128)]
        twins += [lax.ppermute(x, "dp", [(d, d ^ 1) for d in every]) for x in late[1:]]
        last = pl.pallas_call(
            write_last,
            out_shape=jax.ShapeDtypeStruct(most[2].shape, bf16),
            in_specs=[in_hbm, in_vmem],
            out_specs=in_hbm,
            scratch_shapes=[dma],
            input_output_aliases={0: 0},
            compiler_params=grant,
            cost_estimate=pl.CostEstimate(flops=MOST_COST // 16, bytes_accessed=7 * 10**6, transcendentals=0),
        )(most[2], last_w)
        last = pl.pallas_call(
            write_late,
            out_shape=jax.ShapeDtypeStruct(last.shape, bf16),
            in_specs=[in_hbm] + [in_vmem] * (2 * CHIPS),
            out_specs=in_hbm,
            scratch_shapes=[dma((2 * CHIPS,))],
            input_output_aliases={0: 0},
            compiler_params=grant,
        )(last, *late, *twins)
        outs = [*(x.reshape(layers, -1, 128) for x in (most[0], most[1], last)), *most[3:]]
        outs = [untiles(o, *old.shape[1:]) for o, old in zip(outs, (*weights, *m, *v), strict=True)]
        return tuple(outs)

    all_of, cut = P(None, None, None), P(None, "dp", None)
    return jax.shard_map(
        step,
        mesh=mesh,
        in_specs=(P(("rep", "dp"), None, None, None),) * 3 + (all_of,) * 3 + (cut,) * 6,
        out_specs=(P("rep", None, None),) * 3 + (P("rep", "dp", None),) * 6,
        check_vma=False,
    )
```
